128 devices in a mesh: section: 2 (over core), expert: 64 (over x, z, y).
Axes of the slice: x: 4, y: 4, z: 4, core: 2. Of those that a mesh axis runs over, the one named last changes fastest.
Arguments:
- grad_out: bfloat16 [2, 8192, 4096], P('section', 'expert'), may hold values from -6 to 6
- saved_hidden: bfloat16 [2, 8192, 8, 1024], P('section', 'expert'), may hold values from -6 to 6
- routes: int32 [2, 8192, 8], P('section', 'expert'), may hold values from 0 to 63, all different within a row; in each aligned block of 128 rows (0 to 127, 128 to 255, ..., all dimensions but the last counted through in order) at most 24 rows name the same one
- scores: float32 [2, 8192, 8], P('section', 'expert'), may hold values from 0.02 to 0.98
- down_weight: bfloat16 [2, 64, 1024, 4096], P('section', 'expert'), may hold values from -0.1875 to 0.1875
- router: bfloat16 [2, 64, 4096], P('section'), may hold values from -0.59765625 to 0.59765625
Outputs:
- weight_grad: bfloat16 [2, 64, 1024, 4096], P('section', 'expert')
- handed: bfloat16 [2, 8192, 4096], P('section', 'expert')
The draws below stay inside these ranges and needn't reach their ends.
Inputs may be any that keep to these rules, and one draw needn't show every extreme that they name: `routes`: each token names 8 different experts. Among the 128 tokens of one index of expert (aligned blocks), no expert is named more than 24 times, and in every draw some expert is named exactly 24 times in some block.
All inputs are finite; a program needn't handle non-finite values.
Results may differ from the reference program's by a relative error of at most 0.007.
Values may be sent and summed in bfloat16 or wider, within the bound.
A program may use at most 128 MiB of HBM per device.

```python
import math
import jax
import jax.numpy as jnp
import numpy as np
from jax import lax

D = 4096
FF = 1024
TOP = 8
TOK_DEV = 128
SECTIONS = 2
EXPERTS = 64
TOKENS = 8192
CAP = 24


def levels(stream_key, dims, shards, smallest, high):
    gain, own = 1.0, jax.random.fold_in(stream_key, 6)
    for axis_at, shards_of in shards:
        heights = jnp.exp(jax.random.uniform(jax.random.fold_in(own, axis_at), (shards_of,), jnp.float32, smallest / len(shards), high / len(shards)))
        gain = gain * jnp.repeat(heights, dims[axis_at] // shards_of).reshape([-1 if axis == axis_at else 1 for axis in range(len(dims))])
    return gain


def deal_out(stream_key, own, number, rows, amount, top, bound, skew):
    sequence = jax.random.permutation(stream_key, amount)
    packed, ordinary = load_shares(amount, rows * top, bound, skew, True), load_shares(amount, rows * top, bound, skew, False)
    places = jnp.arange(amount)

    def named(lengths, offset_by):
        used = int((lengths > 0).sum())
        fixed = max(1, used // 4)
        moved = fixed + (places - fixed + offset_by * (used - fixed)) % max(1, amount - fixed)
        return jnp.zeros((amount,), jnp.int32).at[sequence[jnp.where(places < fixed, places, moved)]].set(jnp.asarray(lengths, jnp.int32))

    lengths = jnp.where(number % 4 == 0, named(packed, number // 4), named(ordinary, number - number // 4 - 1))
    mixed = jax.random.permutation(jax.random.fold_in(own, 3), amount)
    source_of, sink = mixed[0:amount // 2 * 2:2], mixed[1:amount // 2 * 2:2]
    room = jnp.minimum(lengths[source_of] - 1, bound - lengths[sink]) // 2
    room = jnp.where((source_of == sequence[0]) | (sink == sequence[0]) | (lengths[sink] == 0), 0, jnp.maximum(room, 0))
    moved = jax.random.randint(jax.random.fold_in(own, 4), (amount // 2,), 0, 1 << 20) % (room + 1)
    lengths = lengths.at[source_of].add(-moved).at[sink].add(moved)
    items = jnp.searchsorted(jnp.cumsum(lengths), jnp.arange(rows * top), side="right").astype(jnp.int32)
    table = items.reshape(top, rows).T
    table = table[jax.random.permutation(jax.random.fold_in(own, 1), rows)]
    offset_by = jax.random.randint(jax.random.fold_in(own, 2), (rows, 1), 0, top)
    return jnp.take_along_axis(table, (jnp.arange(top)[None, :] + offset_by) % top, axis=1)


def load_shares(count, total, most, slope, full):
    portions = [(1 << 20) // math.isqrt(grade ** slope) + 1 for grade in range(1, count + 1)]
    largest = most if full else min(most, max(-(-total // count), total * portions[0] // sum(portions)))
    least = 1 if total - largest >= count - 1 else 0
    holding, rest = [largest] + [least] * (count - 1), total - largest - least * (count - 1)
    while rest > 0:
        free = [i for i in range(1, count) if holding[i] < largest] or [i for i in range(1, count) if holding[i] < most]
        mass, budget = sum([portions[i] for i in free]), rest
        for i in free:
            extra = min(most - holding[i], max(1, budget * portions[i] // mass), rest)
            holding[i] = holding[i] + extra
            rest = rest - extra
    return np.array(holding)


def centred(own_key, extent, width, most, shards=(), kind=jnp.bfloat16):
    result = jax.random.normal(own_key, extent, jnp.float32) * width
    if len(shards) > 0:
        result = levels(own_key, extent, shards, -0.22, 0.18) * result
    return jnp.clip(result, min=-most, max=most).astype(kind)


def setup_inputs(seed: int = 0) -> dict:
    key_of = jax.random.split(jax.random.key(seed), 7)
    grad_out = centred(key_of[0], (SECTIONS, TOKENS, D), 1.0, 6.0, ((0, 2), (1, 64)))
    saved_hidden = centred(key_of[1], (SECTIONS, TOKENS, TOP, FF), 1.0, 6.0, ((0, 2), (1, 64)))
    routes_keys = jax.random.split(jax.random.fold_in(key_of[2], 1), SECTIONS * TOKENS // TOK_DEV)
    routes_turns = jax.random.permutation(jax.random.fold_in(key_of[2], 3), SECTIONS * TOKENS // TOK_DEV)
    routes = jax.vmap(lambda own, number: deal_out(jax.random.fold_in(key_of[2], 2), own, number, TOK_DEV, EXPERTS, TOP, CAP, 2))(routes_keys, routes_turns).reshape((SECTIONS, TOKENS, TOP))
    scores = jnp.clip(0.02 + 0.96000002 * jax.random.uniform(key_of[3], (SECTIONS, TOKENS, TOP), jnp.float32) ** levels(key_of[3], (SECTIONS, TOKENS, TOP), ((0, 2), (1, 64)), -0.2, 0.2), 0.02, 0.98)
    down_weight = centred(key_of[4], (SECTIONS, EXPERTS, FF, D), FF ** -0.5, 0.1875, ((0, 2), (1, 64)))
    router = centred(key_of[5], (SECTIONS, EXPERTS, D), 0.1, 0.59765625, ((0, 2),))
    return dict(grad_out=grad_out, saved_hidden=saved_hidden, routes=routes, scores=scores, down_weight=down_weight, router=router)


def slot_rows(route_ids, n_experts, per_block, capacity):
    flat_routes = route_ids.reshape(-1)
    entries = flat_routes.shape[0]
    n_blocks = entries // per_block
    onehot = (flat_routes[:, None] == jnp.arange(n_experts, dtype=jnp.int32)[None, :]).astype(jnp.int32)
    running = jnp.cumsum(onehot.reshape(n_blocks, per_block, n_experts), axis=1).astype(jnp.int32)
    running = running.reshape(entries, n_experts)
    slot_index = jnp.sum(running * onehot, axis=1).astype(jnp.int32) - 1
    block_index = jnp.arange(entries, dtype=jnp.int32) // per_block
    row_index = (block_index * capacity + slot_index).astype(jnp.int32)
    source = jnp.full((n_experts, n_blocks * capacity), entries, jnp.int32)
    source = source.at[flat_routes, row_index].set(jnp.arange(entries, dtype=jnp.int32))
    return flat_routes, row_index, source


def section_pass(grad_rows, hidden_rows, route_ids, score_rows, down_all, router_rows):
    n_tokens, n_routes = route_ids.shape
    n_experts = router_rows.shape[0]
    entries = n_tokens * n_routes
    flat_routes, row_index, source = slot_rows(route_ids, n_experts, TOK_DEV * n_routes, CAP)
    score_total = jnp.sum(score_rows, axis=1, keepdims=True)
    weights = score_rows / score_total
    weights_low = weights.astype(jnp.bfloat16).reshape(-1)
    hidden_flat = hidden_rows.reshape(entries, hidden_rows.shape[2])

    def one_expert(operands):
        slot_source, expert_down = operands
        filled = slot_source < entries
        safe_index = jnp.minimum(slot_source, entries - 1)
        grad_in = jnp.where(filled[:, None], grad_rows[safe_index // n_routes], jnp.zeros((), jnp.bfloat16))
        hidden_in = jnp.where(filled[:, None], hidden_flat[safe_index], jnp.zeros((), jnp.bfloat16))
        weight_in = jnp.where(filled, weights_low[safe_index], jnp.zeros((), jnp.bfloat16))
        projected = lax.dot_general(grad_in, expert_down, (((1,), (1,)), ((), ())), preferred_element_type=jnp.float32)
        derivs = jnp.sum(projected * hidden_in.astype(jnp.float32), axis=1)
        scaled = (weight_in.astype(jnp.float32)[:, None] * grad_in.astype(jnp.float32)).astype(jnp.bfloat16)
        weight_grads = lax.dot_general(hidden_in, scaled, (((0,), (0,)), ((), ())), preferred_element_type=jnp.float32)
        return weight_grads.astype(jnp.bfloat16), derivs

    weight_grads, derivs = lax.map(one_expert, (source, down_all))
    derivs_home = derivs[flat_routes, row_index].reshape(n_tokens, n_routes)
    center = jnp.sum(weights * derivs_home, axis=1, keepdims=True)
    logit_grad = score_rows * (1.0 - score_rows) / score_total * (derivs_home - center)
    expert_ids = jnp.arange(n_experts, dtype=jnp.int32)
    dense_grad = jnp.sum(jnp.where(route_ids[:, :, None] == expert_ids[None, None, :], logit_grad[:, :, None], 0.0), axis=1)
    input_grad = grad_rows.astype(jnp.float32) + jnp.dot(dense_grad, router_rows.astype(jnp.float32), precision=lax.Precision.HIGHEST)
    return weight_grads, input_grad.astype(jnp.bfloat16)


def reference(grad_out, saved_hidden, routes, scores, down_weight, router):
    weight_list = []
    input_list = []
    for section_index in range(SECTIONS):
        weight_grads, input_grad = section_pass(grad_out[section_index], saved_hidden[section_index], routes[section_index], scores[section_index], down_weight[section_index], router[section_index])
        weight_list.append(weight_grads)
        input_list.append(input_grad)
    handed = jnp.roll(jnp.stack(input_list), -1, axis=0)
    return jnp.stack(weight_list), handed
```

```python
import functools
import jax
import jax.numpy as jnp
from jax import lax
from jax.experimental import pallas as pl
from jax.experimental.pallas import tpu as pltpu
from jax.sharding import PartitionSpec as P

MESH = pl.DeviceIdType.MESH
CAP = 24
ORDERS = ((0, 1, 2), (1, 2, 0), (2, 0, 1))
STRIDE = (16, 4, 1)
GB = (11, 11, 10)
HB = (2, 3, 3)


def starts(blocks):
    return tuple(128 * sum(blocks[:i]) for i in range(len(blocks)))


def comm_kernel(grad, rt, hid, tgt, wgt, F, HR,
                gb0, gb1, gb2, sc0, sc1, sc2, ha0, ha1, ha2, hb0, hb1, hb2, hc0, hc1, hc2,
                lsem, gas, gar, gbs, gbr, gcs, gcr, gcl, has, har, hbs, hbr, hcs, hcr, hcl):
    gb, sc, ha, hb, hc = (gb0, gb1, gb2), (sc0, sc1, sc2), (ha0, ha1, ha2), (hb0, hb1, hb2), (hc0, hc1, hc2)
    e = lax.axis_index("expert")
    co = (e // 16, (e // 4) % 4, e % 4)
    gcol, hcol = starts(GB), starts(HB)

    def wrap(v):
        return lax.rem(v + 4, 4)

    def peer(axis, delta):
        c = list(co)
        c[axis] = wrap(co[axis] + delta)
        return {"expert": c[0] * 16 + c[1] * 4 + c[2]}

    def rcopy(src, dst, ss, rs, axis, delta):
        return pltpu.make_async_remote_copy(src_ref=src, dst_ref=dst, send_sem=ss, recv_sem=rs,
                                            device_id=peer(axis, delta), device_id_type=MESH)

    sends = []

    def go(cp):
        cp.start()
        sends.append(cp)
        return cp

    loads = []
    for p, (A, B, C) in enumerate(ORDERS):
        gw = GB[p] * 128
        own = gb[p].at[co[B], co[A]]
        l0 = pltpu.make_async_copy(grad.at[:, pl.ds(gcol[p], gw)], own.at[:, pl.ds(0, gw)], lsem.at[p, 0])
        l1 = pltpu.make_async_copy(rt, own.at[:, pl.ds(gw, 128)], lsem.at[p, 1])
        l0.start(); l1.start()
        loads.append((l0, l1))

    def ring(p, axis, slot_of, sems, semr, idx):
        gw = GB[p] * 128 + 128
        half = (gw // 256) * 128
        def cp(i, src_delta, cols, delta):
            ref = slot_of(src_delta)
            if cols is not None:
                ref = ref.at[:, pl.ds(*cols)]
            return rcopy(ref, ref, sems.at[idx + (i,)], semr.at[idx + (i,)], axis, delta)
        return (cp(0, 0, None, 1), cp(1, 0, None, -1), cp(2, -1, (0, half), 1), cp(3, 1, (half, gw - half), -1))

    acp, bcp = [], {}
    for p, (A, B, C) in enumerate(ORDERS):
        acp.append(ring(p, A, lambda d, p=p, A=A, B=B: gb[p].at[co[B], wrap(co[A] + d)], gas, gar, (p,)))
        for k, da in enumerate((0, -1, 1, 2)):
            bcp[p, k] = ring(p, B, lambda d, p=p, A=A, B=B, da=da: gb[p].at[wrap(co[B] + d), wrap(co[A] + da)], gbs, gbr, (p, k))
    for p in range(3):
        loads[p][0].wait(); loads[p][1].wait()
        go(acp[p][0]); go(acp[p][1])
    for p in range(3):
        go(bcp[p, 0][0]); go(bcp[p, 0][1])

    for p, (A, B, C) in enumerate(ORDERS):
        hw = HB[p] * 128
        r = lax.broadcasted_iota(jnp.int32, (16 * CAP, 1), 0)
        dB = (r >= 4 * CAP).astype(jnp.int32) + (r >= 8 * CAP).astype(jnp.int32) + (r >= 12 * CAP).astype(jnp.int32)
        r1 = r - dB * (4 * CAP)
        dC = (r1 >= CAP).astype(jnp.int32) + (r1 >= 2 * CAP).astype(jnp.int32) + (r1 >= 3 * CAP).astype(jnp.int32)
        slot = r1 - dC * CAP
        base = CAP * (dB * STRIDE[B] + dC * STRIDE[C]) + slot
        for d in (1, 3, 2, 0):
            code = base + CAP * STRIDE[A] * wrap(co[A] + d)
            pick = jnp.where(code == tgt[...], wgt[...], 0.0).astype(jnp.bfloat16)
            rows = jnp.dot(pick, hid[:, hcol[p]:hcol[p] + hw], preferred_element_type=jnp.float32)
            rows = rows.reshape(4, 4, CAP, hw).astype(jnp.bfloat16)
            if d == 0:
                for j in range(4):
                    hb[p][j, co[A]] = rows[j]
            else:
                ha[p][d - 1] = rows
                go(rcopy(ha[p].at[d - 1], hb[p].at[:, co[A]], has.at[p, d - 1], har.at[p, d - 1], A, d))
    hacp = {}
    for p, (A, B, C) in enumerate(ORDERS):
        for d in (1, 2, 3):
            hacp[p, d] = rcopy(ha[p].at[d - 1], hb[p].at[:, wrap(co[A] - d)], has.at[p, d - 1], har.at[p, d - 1], A, d)

    for p in range(3):
        acp[p][0].wait_recv(); go(acp[p][2])
        acp[p][1].wait_recv(); go(acp[p][3])
    for p in range(3):
        for k in (1, 2):
            go(bcp[p, k][0]); go(bcp[p, k][1])
    for p in range(3):
        acp[p][2].wait_recv(); acp[p][3].wait_recv()
        go(bcp[p, 3][0]); go(bcp[p, 3][1])

    j = lax.broadcasted_iota(jnp.int32, (4 * CAP, 1), 0)
    dCj = (j >= CAP).astype(jnp.int32) + (j >= 2 * CAP).astype(jnp.int32) + (j >= 3 * CAP).astype(jnp.int32)
    slotj = (j - dCj * CAP).astype(jnp.float32)
    lane = lax.broadcasted_iota(jnp.int32, (4 * CAP, 64), 1)

    def pack(p, db):
        A, B, C = ORDERS[p]
        gw = GB[p] * 128
        cc = co[C] + dCj
        cc = jnp.where(cc >= 4, cc - 4, cc)
        eid = STRIDE[A] * co[A] + STRIDE[B] * co[B] + STRIDE[C] * cc
        E = jnp.where(lane == eid, 1.0, 0.0).astype(jnp.bfloat16)
        bb = wrap(co[B] + db)

        def one(a, carry):
            codes = jnp.dot(E, gb[p][bb, a, 0:64, gw:gw + 128], preferred_element_type=jnp.float32)
            sel = jnp.where(codes == slotj, 1.0, 0.0).astype(jnp.bfloat16)
            rows = jnp.dot(sel, gb[p][bb, a, :, 0:gw], preferred_element_type=jnp.float32)
            rows = rows.reshape(4, CAP, gw).astype(jnp.bfloat16)
            for dc in range(4):
                sc[p][dc, db % 4, a] = rows[dc]
            return carry
        lax.fori_loop(0, 4, one, 0)
        for dc in (1, 3, 2):
            go(rcopy(sc[p].at[dc, db % 4], fdst(p, bb, 0), gcs.at[p, db % 4, dc - 1], gcr.at[p, db % 4, dc - 1], C, dc))
        cp = pltpu.make_async_copy(sc[p].at[0, db % 4], fdst(p, bb, 0), gcl.at[p, db % 4])
        cp.start()
        locals_.append(cp)

    def fdst(p, bb, d):
        A, B, C = ORDERS[p]
        idx = [None, None, None]
        idx[A] = slice(None)
        idx[B] = bb
        idx[C] = wrap(co[C] - d)
        return F.at[idx[0], idx[1], idx[2], :, pl.ds(gcol[p], GB[p] * 128)]

    def hdst(p, bb, d):
        A, B, C = ORDERS[p]
        idx = [None, None, None]
        idx[A] = slice(None)
        idx[B] = bb
        idx[C] = wrap(co[C] - d)
        return HR.at[idx[0], idx[1], idx[2], :, pl.ds(hcol[p], HB[p] * 128)]

    locals_ = []
    hbcp = {}
    for p, (A, B, C) in enumerate(ORDERS):
        for d in (1, 3, 2):
            hacp[p, d].wait_recv()
        for d in (1, 3, 2):
            hbcp[p, d] = go(rcopy(hb[p].at[wrap(co[B] + d)], hc[p].at[d - 1], hbs.at[p, d - 1], hbr.at[p, d - 1], B, d))
    for p in range(3):
        pack(p, 0)
    for k in range(4):
        for p in range(3):
            bcp[p, k][0].wait_recv(); go(bcp[p, k][2])
            bcp[p, k][1].wait_recv(); go(bcp[p, k][3])

    def hidden_c(p, d):
        A, B, C = ORDERS[p]
        bb = wrap(co[B] - d)
        for dc in (1, 3, 2, 0):
            cs = wrap(co[C] + dc)
            src = hb[p].at[co[B], :, cs] if d == 0 else hc[p].at[d - 1, :, cs]
            if dc == 0:
                cp = pltpu.make_async_copy(src, hdst(p, bb, 0), hcl.at[p, d])
                cp.start()
                locals_.append(cp)
            else:
                go(rcopy(src, hdst(p, bb, 0), hcs.at[p, d, dc - 1], hcr.at[p, d, dc - 1], C, dc))
    for p in range(3):
        hidden_c(p, 0)
    for p in range(3):
        pack(p, -1)
    for p in range(3):
        pack(p, 1)
    for p in range(3):
        for d in (1, 3, 2):
            hbcp[p, d].wait_recv()
            hidden_c(p, d)
    for p in range(3):
        for k in range(4):
            bcp[p, k][2].wait_recv(); bcp[p, k][3].wait_recv()
        pack(p, 2)
    for p, (A, B, C) in enumerate(ORDERS):
        for db in (0, -1, 1, 2):
            bb = wrap(co[B] + db)
            for dc in (1, 3, 2):
                rcopy(sc[p].at[dc, db % 4], fdst(p, bb, dc), gcs.at[p, db % 4, dc - 1], gcr.at[p, db % 4, dc - 1], C, dc).wait_recv()
        for d in range(4):
            for dc in (1, 3, 2):
                src = hc[p].at[max(d - 1, 0), :, 0]
                rcopy(src, hdst(p, wrap(co[B] - d), dc), hcs.at[p, d, dc - 1], hcr.at[p, d, dc - 1], C, dc).wait_recv()
    for cp in locals_:
        cp.wait()
    for cp in sends:
        cp.wait_send()


def exchange(grad, rt, hid, tgt, wgt):
    bf = jnp.bfloat16
    V = pltpu.VMEM
    D = pltpu.SemaphoreType.DMA
    any_ = pl.BlockSpec(memory_space=pl.ANY)
    vm = pl.BlockSpec(memory_space=pltpu.VMEM)
    F, HR = pl.pallas_call(
        comm_kernel,
        out_shape=(jax.ShapeDtypeStruct((4, 4, 4, CAP, 4096), bf), jax.ShapeDtypeStruct((4, 4, 4, CAP, 1024), bf)),
        in_specs=[any_, any_, vm, vm, vm], out_specs=(any_, any_),
        scratch_shapes=[V((4, 4, 128, g * 128 + 128), bf) for g in GB]
        + [V((4, 4, 4, CAP, g * 128), bf) for g in GB]
        + [V((3, 4, 4, CAP, h * 128), bf) for h in HB]
        + [V((4, 4, 4, CAP, h * 128), bf) for h in HB]
        + [V((3, 4, 4, CAP, h * 128), bf) for h in HB]
        + [D((3, 2)), D((3, 4)), D((3, 4)), D((3, 4, 4)), D((3, 4, 4)), D((3, 4, 3)), D((3, 4, 3)), D((3, 4)),
           D((3, 3)), D((3, 3)), D((3, 3)), D((3, 3)), D((3, 4, 3)), D((3, 4, 3)), D((3, 4))],
        compiler_params=pltpu.CompilerParams(has_side_effects=True, vmem_limit_bytes=62 * 2**20),
    )(grad, rt, hid, tgt, wgt)
    return F.reshape(64 * CAP, 4096), HR.reshape(64 * CAP, 1024)


def body(grad_out, saved_hidden, routes, scores, down_weight, router):
    grad_rows, route_ids, score_rows = grad_out[0], routes[0], scores[0]
    expert_down, router_rows = down_weight[0, 0], router[0]
    n_tokens, n_routes, hidden_width = saved_hidden.shape[1:]
    n_experts = router_rows.shape[0]
    hidden_flat = saved_hidden[0].reshape(n_tokens * n_routes, hidden_width)
    ids = jnp.arange(n_experts, dtype=jnp.int32)
    onehot = (route_ids[:, :, None] == ids).astype(jnp.float32)
    member = jnp.sum(onehot, axis=1)
    t = jnp.arange(n_tokens, dtype=jnp.int32)
    tril = (t[:, None] > t[None, :]).astype(jnp.bfloat16)
    rank = jnp.dot(tril, member.astype(jnp.bfloat16), preferred_element_type=jnp.float32)
    code = jnp.where(member > 0, rank, -1.0)
    rt = jnp.zeros((128, 128), jnp.bfloat16).at[:n_experts].set(code.T.astype(jnp.bfloat16))
    slot = jnp.sum(onehot * rank[:, None, :], axis=2).astype(jnp.int32)
    target = route_ids * CAP + slot
    total = jnp.sum(score_rows, axis=1, keepdims=True)
    weights = score_rows / total
    low = weights.astype(jnp.bfloat16).astype(jnp.float32)
    grad_recv, hidden_recv = exchange(grad_rows, rt, hidden_flat, target.reshape(1, -1), low.reshape(1, -1))
    proj = lax.dot_general(grad_recv, expert_down, (((1,), (1,)), ((), ())), preferred_element_type=jnp.float32)
    derivs = jnp.sum(proj * hidden_recv.astype(jnp.float32), axis=1)
    back = lax.all_to_all(derivs.reshape(n_experts, CAP), "expert", split_axis=0, concat_axis=0, tiled=True)
    weight_out = lax.dot_general(hidden_recv, grad_recv, (((0,), (0,)), ((), ())), preferred_element_type=jnp.float32).astype(jnp.bfloat16)
    home = jnp.zeros((n_tokens, n_experts), jnp.float32)
    for s in range(CAP):
        home = home + jnp.where(code == s, back[:, s][None, :], 0.0)
    rd = jnp.sum(onehot * home[:, None, :], axis=2) / low
    center = jnp.sum(weights * rd, axis=1, keepdims=True)
    logit = score_rows * (1.0 - score_rows) / total * (rd - center)
    dense = jnp.sum(onehot * logit[:, :, None], axis=1)
    inp = grad_rows.astype(jnp.float32) + jnp.dot(dense, router_rows.astype(jnp.float32))
    handed = lax.ppermute(inp.astype(jnp.bfloat16), "section", [(0, 1), (1, 0)])
    return weight_out[None, None], handed[None]


def solution(mesh):
    return jax.shard_map(
        body, mesh=mesh,
        in_specs=(P("section", "expert", None), P("section", "expert", None, None), P("section", "expert", None),
                  P("section", "expert", None), P("section", "expert", None, None), P("section", None, None)),
        out_specs=(P("section", "expert", None, None), P("section", "expert", None)), check_vma=False)
```

```python
import functools
import jax
import jax.numpy as jnp
from jax import lax
from jax.experimental import pallas as pl
from jax.experimental.pallas import tpu as pltpu
from jax.sharding import PartitionSpec as P

MESH = pl.DeviceIdType.MESH
CAP = 24
ORDERS = ((0, 1, 2), (1, 2, 0), (2, 0, 1))
STRIDE = (16, 4, 1)
GB = (10, 12, 10)
HB = (2, 3, 3)


def starts(blocks):
    return tuple(128 * sum(blocks[:i]) for i in range(len(blocks)))


def comm_kernel(routes, scores, router, grad, hidden, down, F, HR, handed, hid, HV, wv, gch, g2, ds, dr, hnd, codes_s, score_s,
                gb0, gb1, gb2, sc0, sc1, sc2, ha0, ha1, ha2, hb0, hb1, hb2, hc0, hc1, hc2,
                lsem, gas, gar, gbs, gbr, gcs, gcr, gcl, has, har, hbs, hbr, hcs, hcr, gls, wsem, dss, drs, hos, hns, hnr):
    gb, sc, ha, hb, hc = (gb0, gb1, gb2), (sc0, sc1, sc2), (ha0, ha1, ha2), (hb0, hb1, hb2), (hc0, hc1, hc2)
    e = lax.axis_index("expert")
    co = (e // 16, (e // 4) % 4, e % 4)
    gcol, hcol = starts(GB), starts(HB)

    def wrap(v):
        return lax.rem(v + 4, 4)

    def peer(axis, delta):
        c = list(co)
        c[axis] = wrap(co[axis] + delta)
        return {"expert": c[0] * 16 + c[1] * 4 + c[2]}

    def rcopy(src, dst, ss, rs, axis, delta):
        return pltpu.make_async_remote_copy(src_ref=src, dst_ref=dst, send_sem=ss, recv_sem=rs,
                                            device_id=peer(axis, delta), device_id_type=MESH)

    sends = []

    def go(cp):
        cp.start()
        sends.append(cp)
        return cp

    loads = []
    for p, (A, B, C) in enumerate(ORDERS):
        gw = GB[p] * 128
        own = gb[p].at[co[B], co[A]]
        l0 = pltpu.make_async_copy(grad.at[:, pl.ds(gcol[p], gw)], own.at[:, pl.ds(0, gw)], lsem.at[p, 0])
        l0.start()
        loads.append(l0)
    hload = pltpu.make_async_copy(hidden, hid, lsem.at[0, 1])
    hload.start()
    wload = pltpu.make_async_copy(down, wv, wsem.at[0])
    wload.start()

    f32, bf = jnp.float32, jnp.bfloat16
    ri = jnp.transpose(routes[...].astype(f32))
    st = jnp.transpose(scores[...])
    tot = jnp.sum(st, axis=0, keepdims=True)
    low = (st / tot).astype(bf)
    eio = lax.broadcasted_iota(jnp.int32, (64, 128), 0).astype(f32)
    member = jnp.zeros((64, 128), f32)
    score_e = jnp.zeros((64, 128), f32)
    for k in range(8):
        hit = eio == ri[k:k + 1, :]
        member = member + jnp.where(hit, 1.0, 0.0)
        score_e = score_e + jnp.where(hit, st[k:k + 1, :], 0.0)
    before = lax.broadcasted_iota(jnp.int32, (128, 128), 0) < lax.broadcasted_iota(jnp.int32, (128, 128), 1)
    rank = jnp.dot(member.astype(bf), jnp.where(before, 1.0, 0.0).astype(bf), preferred_element_type=f32)
    code_e = jnp.where(member > 0.0, rank, -1.0)
    codes_s[...] = code_e
    score_s[...] = score_e
    code_b = jnp.concatenate([code_e, jnp.full((64, 128), -1.0, f32)], axis=0).astype(bf)
    for p, (A, B, C) in enumerate(ORDERS):
        gb[p][co[B], co[A], :, GB[p] * 128:GB[p] * 128 + 128] = code_b

    def ring(p, axis, slot_of, sems, semr, idx):
        gw = GB[p] * 128 + 128
        half = (gw // 256) * 128
        def cp(i, src_delta, cols, delta):
            ref = slot_of(src_delta)
            if cols is not None:
                ref = ref.at[:, pl.ds(*cols)]
            return rcopy(ref, ref, sems.at[idx + (i,)], semr.at[idx + (i,)], axis, delta)
        return (cp(0, 0, None, 1), cp(1, 0, None, -1), cp(2, -1, (0, half), 1), cp(3, 1, (half, gw - half), -1))

    acp, bcp = [], {}
    for p, (A, B, C) in enumerate(ORDERS):
        acp.append(ring(p, A, lambda d, p=p, A=A, B=B: gb[p].at[co[B], wrap(co[A] + d)], gas, gar, (p,)))
        for k, da in enumerate((0, -1, 1, 2)):
            bcp[p, k] = ring(p, B, lambda d, p=p, A=A, B=B, da=da: gb[p].at[wrap(co[B] + d), wrap(co[A] + da)], gbs, gbr, (p, k))
    for p in range(3):
        loads[p].wait()
        go(acp[p][0]); go(acp[p][1])
    for p in range(3):
        go(bcp[p, 0][0]); go(bcp[p, 0][1])

    slots = jnp.concatenate([jnp.sum(jnp.where(eio == ri[k:k + 1, :], rank, 0.0), axis=0, keepdims=True) for k in range(8)], axis=0)
    n8 = lax.broadcasted_iota(jnp.int32, (128, 1024), 1) // 8
    spread = jnp.where(n8 == lax.broadcasted_iota(jnp.int32, (128, 1024), 0), 1.0, 0.0).astype(bf)
    mine = lax.broadcasted_iota(jnp.int32, (8, 1024), 1) % 8 == lax.broadcasted_iota(jnp.int32, (8, 1024), 0)

    def lanes(v):
        return jnp.sum(jnp.where(mine, jnp.dot(v.astype(bf), spread, preferred_element_type=f32), 0.0), axis=0, keepdims=True)
    tgt = CAP * lanes(ri) + lanes(slots)
    wgt = lanes(low)
    hload.wait()

    for p, (A, B, C) in enumerate(ORDERS):
        hw = HB[p] * 128
        r = lax.broadcasted_iota(jnp.int32, (16 * CAP, 1), 0)
        dB = (r >= 4 * CAP).astype(jnp.int32) + (r >= 8 * CAP).astype(jnp.int32) + (r >= 12 * CAP).astype(jnp.int32)
        r1 = r - dB * (4 * CAP)
        dC = (r1 >= CAP).astype(jnp.int32) + (r1 >= 2 * CAP).astype(jnp.int32) + (r1 >= 3 * CAP).astype(jnp.int32)
        slot = r1 - dC * CAP
        base = CAP * (dB * STRIDE[B] + dC * STRIDE[C]) + slot
        for d in (1, 3, 2, 0):
            code = base + CAP * STRIDE[A] * wrap(co[A] + d)
            pick = jnp.where(code.astype(f32) == tgt, wgt, 0.0).astype(jnp.bfloat16)
            rows = jnp.dot(pick, hid[:, hcol[p]:hcol[p] + hw], preferred_element_type=jnp.float32)
            rows = rows.reshape(4, 4, CAP, hw).astype(jnp.bfloat16)
            if d == 0:
                for j in range(4):
                    hb[p][j, co[A]] = rows[j]
            else:
                ha[p][d - 1] = rows
                go(rcopy(ha[p].at[d - 1], hb[p].at[:, co[A]], has.at[p, d - 1], har.at[p, d - 1], A, d))
    hacp = {}
    for p, (A, B, C) in enumerate(ORDERS):
        for d in (1, 2, 3):
            hacp[p, d] = rcopy(ha[p].at[d - 1], hb[p].at[:, wrap(co[A] - d)], has.at[p, d - 1], har.at[p, d - 1], A, d)

    for p in range(3):
        acp[p][0].wait_recv(); go(acp[p][2])
        acp[p][1].wait_recv(); go(acp[p][3])
    for p in range(3):
        for k in (1, 2):
            go(bcp[p, k][0]); go(bcp[p, k][1])
    for p in range(3):
        acp[p][2].wait_recv(); acp[p][3].wait_recv()
        go(bcp[p, 3][0]); go(bcp[p, 3][1])

    j = lax.broadcasted_iota(jnp.int32, (4 * CAP, 1), 0)
    dCj = (j >= CAP).astype(jnp.int32) + (j >= 2 * CAP).astype(jnp.int32) + (j >= 3 * CAP).astype(jnp.int32)
    slotj = (j - dCj * CAP).astype(jnp.float32)
    lane = lax.broadcasted_iota(jnp.int32, (4 * CAP, 64), 1)

    def pack(p, db):
        A, B, C = ORDERS[p]
        gw = GB[p] * 128
        cc = co[C] + dCj
        cc = jnp.where(cc >= 4, cc - 4, cc)
        eid = STRIDE[A] * co[A] + STRIDE[B] * co[B] + STRIDE[C] * cc
        E = jnp.where(lane == eid, 1.0, 0.0).astype(jnp.bfloat16)
        bb = wrap(co[B] + db)

        def one(a, carry):
            codes = jnp.dot(E, gb[p][bb, a, 0:64, gw:gw + 128], preferred_element_type=jnp.float32)
            sel = jnp.where(codes == slotj, 1.0, 0.0).astype(jnp.bfloat16)
            rows = jnp.dot(sel, gb[p][bb, a, :, 0:gw], preferred_element_type=jnp.float32)
            rows = rows.reshape(4, CAP, gw).astype(jnp.bfloat16)
            for dc in range(4):
                sc[p][dc, db % 4, a] = rows[dc]
            return carry
        lax.fori_loop(0, 4, one, 0)
        for dc in (1, 3, 2):
            go(rcopy(sc[p].at[dc, db % 4], fdst(p, bb, 0), gcs.at[p, db % 4, dc - 1], gcr.at[p, db % 4, dc - 1], C, dc))
        cp = pltpu.make_async_copy(sc[p].at[0, db % 4], fdst(p, bb, 0), gcl.at[p, db % 4])
        cp.start()
        locals_[p, db % 4] = cp

    def fdst(p, bb, d):
        A, B, C = ORDERS[p]
        idx = [None, None, None]
        idx[A] = slice(None)
        idx[B] = bb
        idx[C] = wrap(co[C] - d)
        return F.at[idx[0], idx[1], idx[2], :, pl.ds(gcol[p], GB[p] * 128)]

    def hdst(p, bb, d):
        A, B, C = ORDERS[p]
        idx = [None, None, None]
        idx[A] = slice(None)
        idx[B] = bb
        idx[C] = wrap(co[C] - d)
        return HV.at[idx[0], idx[1], idx[2], :, pl.ds(hcol[p], HB[p] * 128)]

    locals_ = {}
    hbcp = {}
    for p, (A, B, C) in enumerate(ORDERS):
        for d in (1, 3, 2):
            hacp[p, d].wait_recv()
        for d in (1, 3, 2):
            hbcp[p, d] = go(rcopy(hb[p].at[wrap(co[B] + d)], hc[p].at[d - 1], hbs.at[p, d - 1], hbr.at[p, d - 1], B, d))
    for p in range(3):
        pack(p, 0)
    for k in range(4):
        for p in range(3):
            bcp[p, k][0].wait_recv(); go(bcp[p, k][2])
            bcp[p, k][1].wait_recv(); go(bcp[p, k][3])

    def hidden_c(p, d):
        A, B, C = ORDERS[p]
        bb = wrap(co[B] - d)
        for dc in (1, 3, 2, 0):
            cs = wrap(co[C] + dc)
            src = hb[p].at[co[B], :, cs] if d == 0 else hc[p].at[d - 1, :, cs]
            if dc == 0:
                dst = hdst(p, bb, 0)
                for a in range(4):
                    dst[a] = src[a]
            else:
                go(rcopy(src, hdst(p, bb, 0), hcs.at[p, d, dc - 1], hcr.at[p, d, dc - 1], C, dc))
    for p in range(3):
        hidden_c(p, 0)
    for p in range(3):
        pack(p, -1)
    for p in range(3):
        pack(p, 1)
    for p in range(3):
        for d in (1, 3, 2):
            hbcp[p, d].wait_recv()
            hidden_c(p, d)
    for p in range(3):
        for k in range(4):
            bcp[p, k][2].wait_recv(); bcp[p, k][3].wait_recv()
        pack(p, 2)
    for p, (A, B, C) in enumerate(ORDERS):
        for d in range(4):
            for dc in (1, 3, 2):
                src = hc[p].at[max(d - 1, 0), :, 0]
                rcopy(src, hdst(p, wrap(co[B] - d), dc), hcs.at[p, d, dc - 1], hcr.at[p, d, dc - 1], C, dc).wait_recv()
    hout = pltpu.make_async_copy(HV, HR, hos.at[0])
    hout.start()
    wload.wait()

    def rest(p):
        return tuple(ax for ax in range(3) if ax != ORDERS[p][1])

    def at_b(ref, p, bb):
        idx = [slice(None)] * 3
        idx[ORDERS[p][1]] = bb
        return ref.at[idx[0], idx[1], idx[2]]

    chunks = [(p, db) for db in (0, -1, 1, 2) for p in range(3)]

    def load(n):
        p, db = chunks[n]
        C = ORDERS[p][2]
        bb = wrap(co[ORDERS[p][1]] + db)
        for dc in (1, 3, 2):
            rcopy(sc[p].at[dc, db % 4], fdst(p, bb, dc), gcs.at[p, db % 4, dc - 1], gcr.at[p, db % 4, dc - 1], C, dc).wait_recv()
        locals_[p, db % 4].wait()
        gw = GB[p] * 128
        cp = pltpu.make_async_copy(at_b(F, p, bb).at[:, :, :, pl.ds(gcol[p], gw)], gch.at[n % 2, :, :, :, pl.ds(0, gw)], gls.at[n % 2])
        cp.start()
        return cp

    def derive(n):
        p, db = chunks[n]
        gw = GB[p] * 128
        B = ORDERS[p][1]
        bb = wrap(co[B] + db)
        R1, R2 = rest(p)
        for i in range(4):
            g2[i * 96:(i + 1) * 96, 0:gw] = gch[n % 2, i, :, :, 0:gw].astype(f32).reshape(96, gw).astype(bf)
        hview = at_b(HV, p, bb)
        acc = jnp.zeros((384, 128), f32)
        for f in range(4):
            proj = lax.dot_general(g2[:, 0:gw], wv[f * 256:(f + 1) * 256, gcol[p]:gcol[p] + gw], (((1,), (1,)), ((), ())),
                                   preferred_element_type=f32)
            q = proj * hview[:, :, :, f * 256:(f + 1) * 256].astype(f32).reshape(384, 256)
            acc = acc + q[:, 0:128] + q[:, 128:256]
        pad = jnp.concatenate([acc.reshape(16, CAP, 128), jnp.zeros((16, 8, 128), f32)], axis=1).reshape(512, 128)
        row = jnp.sum(jnp.transpose(pad), axis=0, keepdims=True)
        for i in range(4):
            ds[p, db % 4, i] = row[:, i * 128:(i + 1) * 128]
        for d1 in range(4):
            for d2 in range(4):
                i = wrap(co[R1] + d1)
                if (db, d1, d2) == (0, 0, 0):
                    dr[p, e] = ds[p, 0, i]
                    continue
                c = [None] * 3
                c[R1], c[R2], c[B] = i, wrap(co[R2] + d2), bb
                pltpu.make_async_remote_copy(src_ref=ds.at[p, db % 4, i], dst_ref=dr.at[p, e], send_sem=dss.at[p], recv_sem=drs.at[p],
                                             device_id={"expert": c[0] * 16 + c[1] * 4 + c[2]}, device_id_type=MESH).start()

    cur = load(0)
    for n in range(12):
        nxt = load(n + 1) if n < 11 else None
        cur.wait()
        derive(n)
        cur = nxt

    home = jnp.zeros((64, 128), f32)
    window = lax.broadcasted_iota(jnp.int32, (64, 128), 1) // 32
    for p in range(3):
        pltpu.make_async_copy(dr.at[p, pl.ds(0, 63)], dr.at[p, pl.ds(0, 63)], drs.at[p]).wait()
        home = home + jnp.where(window == co[rest(p)[1]], dr[p].reshape(64, 128), 0.0)
    home = home + pltpu.roll(home, 64, 1)
    home = home + pltpu.roll(home, 32, 1)
    code_e = codes_s[...]
    score_e = score_s[...]
    rd = jnp.zeros((64, 128), f32)
    for s in range(CAP):
        rd = rd + jnp.where(code_e == float(s), home[:, s:s + 1], 0.0)
    tot = jnp.sum(score_e, axis=0, keepdims=True)
    weight = score_e / tot
    on = code_e >= 0.0
    rd = jnp.where(on, rd / jnp.where(on, weight.astype(bf).astype(f32), 1.0), 0.0)
    center = jnp.sum(weight * rd, axis=0, keepdims=True)
    logit = score_e * (1.0 - score_e) / tot * (rd - center)
    lt = jnp.transpose(logit).astype(bf)
    other = {"section": 1 - lax.axis_index("section")}
    hcps = []
    for p, (A, B, C) in enumerate(ORDERS):
        gw = GB[p] * 128
        for c0 in range(0, gw, 256):
            add = jnp.dot(lt, router[:, gcol[p] + c0:gcol[p] + c0 + 256], preferred_element_type=f32)
            hnd[:, gcol[p] + c0:gcol[p] + c0 + 256] = (gb[p][co[B], co[A], :, c0:c0 + 256].astype(f32) + add).astype(bf)
        cols = pl.ds(gcol[p], gw)
        cp = pltpu.make_async_remote_copy(src_ref=hnd.at[:, cols], dst_ref=handed.at[:, cols], send_sem=hns.at[p], recv_sem=hnr.at[p],
                                          device_id=other, device_id_type=MESH)
        cp.start()
        hcps.append(cp)
    for p in range(3):
        pltpu.make_async_copy(dr.at[p, pl.ds(0, 63)], dr.at[p, pl.ds(0, 63)], dss.at[p]).wait()
    hout.wait()
    for cp in sends:
        cp.wait_send()
    for cp in hcps:
        cp.wait()


def exchange(routes, scores, router, grad, hidden, down):
    bf, f32 = jnp.bfloat16, jnp.float32
    V = pltpu.VMEM
    D = pltpu.SemaphoreType.DMA
    any_ = pl.BlockSpec(memory_space=pl.ANY)
    vm = pl.BlockSpec(memory_space=pltpu.VMEM)
    gmax = max(GB) * 128
    F, HR, handed = pl.pallas_call(
        comm_kernel,
        out_shape=(jax.ShapeDtypeStruct((4, 4, 4, CAP, 4096), bf), jax.ShapeDtypeStruct((4, 4, 4, CAP, 1024), bf),
                   jax.ShapeDtypeStruct((128, 4096), bf)),
        in_specs=[vm, vm, vm, any_, any_, any_], out_specs=(any_, any_, any_),
        scratch_shapes=[V((1024, 1024), bf), V((4, 4, 4, CAP, 1024), bf), V((1024, 4096), bf), V((2, 4, 4, CAP, gmax), bf),
                        V((384, gmax), bf), V((3, 4, 4, 1, 128), f32), V((3, 64, 1, 128), f32), V((128, 4096), bf),
                        V((64, 128), f32), V((64, 128), f32)]
        + [V((4, 4, 128, g * 128 + 128), bf) for g in GB]
        + [V((4, 4, 4, CAP, g * 128), bf) for g in GB]
        + [V((3, 4, 4, CAP, h * 128), bf) for h in HB]
        + [V((4, 4, 4, CAP, h * 128), bf) for h in HB]
        + [V((3, 4, 4, CAP, h * 128), bf) for h in HB]
        + [D((3, 2)), D((3, 4)), D((3, 4)), D((3, 4, 4)), D((3, 4, 4)), D((3, 4, 3)), D((3, 4, 3)), D((3, 4)),
           D((3, 3)), D((3, 3)), D((3, 3)), D((3, 3)), D((3, 4, 3)), D((3, 4, 3)),
           D((2,)), D((1,)), D((3,)), D((3,)), D((1,)), D((3,)), D((3,))],
        compiler_params=pltpu.CompilerParams(has_side_effects=True, vmem_limit_bytes=63 * 2**20),
    )(routes, scores, router, grad, hidden, down)
    return F.reshape(64 * CAP, 4096), HR.reshape(64 * CAP, 1024), handed


def body(grad_out, saved_hidden, routes, scores, down_weight, router):
    n_tokens, n_routes, hidden_width = saved_hidden.shape[1:]
    hidden_flat = saved_hidden[0].reshape(n_tokens * n_routes, hidden_width)
    grad_recv, hidden_recv, handed = exchange(routes[0], scores[0], router[0], grad_out[0], hidden_flat, down_weight[0, 0])
    weight_out = lax.dot_general(hidden_recv, grad_recv, (((0,), (0,)), ((), ())), preferred_element_type=jnp.float32).astype(jnp.bfloat16)
    return weight_out[None, None], handed[None]


def solution(mesh):
    return jax.shard_map(
        body, mesh=mesh,
        in_specs=(P("section", "expert", None), P("section", "expert", None, None), P("section", "expert", None),
                  P("section", "expert", None), P("section", "expert", None, None), P("section", None, None)),
        out_specs=(P("section", "expert", None, None), P("section", "expert", None)), check_vma=False)
```

```python
import functools
import jax
import jax.numpy as jnp
from jax import lax
from jax.experimental import pallas as pl
from jax.experimental.pallas import tpu as pltpu
from jax.sharding import PartitionSpec as P

MESH = pl.DeviceIdType.MESH
CAP = 24
ORDERS = ((0, 1, 2), (1, 2, 0), (2, 0, 1))
STRIDE = (16, 4, 1)
GB = (10, 12, 10)
HB = (2, 3, 3)


def starts(blocks):
    return tuple(128 * sum(blocks[:i]) for i in range(len(blocks)))


def comm_kernel(routes, scores, router, grad, hidden, down, F, HR, handed, hid, HV, wv, gch, g2, ds, dr, hnd, codes_s, score_s,
                gb0, gb1, gb2, sc0, sc1, sc2, ha0, ha1, ha2, hb0, hb1, hb2, hc0, hc1, hc2,
                lsem, gas, gar, gbs, gbr, gcs, gcr, gcl, has, har, hbs, hbr, hcs, hcr, gls, wsem, dss, drs, hos, hns, hnr):
    gb, sc, ha, hb, hc = (gb0, gb1, gb2), (sc0, sc1, sc2), (ha0, ha1, ha2), (hb0, hb1, hb2), (hc0, hc1, hc2)
    e = lax.axis_index("expert")
    co = (e // 16, (e // 4) % 4, e % 4)
    gcol, hcol = starts(GB), starts(HB)

    def wrap(v):
        return lax.rem(v + 4, 4)

    def peer(axis, delta):
        c = list(co)
        c[axis] = wrap(co[axis] + delta)
        return {"expert": c[0] * 16 + c[1] * 4 + c[2]}

    def rcopy(src, dst, ss, rs, axis, delta):
        return pltpu.make_async_remote_copy(src_ref=src, dst_ref=dst, send_sem=ss, recv_sem=rs,
                                            device_id=peer(axis, delta), device_id_type=MESH)

    other = {"section": 1 - lax.axis_index("section")}
    barrier = pltpu.get_barrier_semaphore()
    for axis in range(3):
        for d in (1, 2, 3):
            pl.semaphore_signal(barrier, inc=1, device_id=peer(axis, d), device_id_type=MESH)
    pl.semaphore_signal(barrier, inc=1, device_id=other, device_id_type=MESH)

    sends = []

    def go(cp):
        cp.start()
        sends.append(cp)
        return cp

    loads = []
    for p, (A, B, C) in enumerate(ORDERS):
        gw = GB[p] * 128
        own = gb[p].at[co[B], co[A]]
        l0 = pltpu.make_async_copy(grad.at[:, pl.ds(gcol[p], gw)], own.at[:, pl.ds(0, gw)], lsem.at[p, 0])
        l0.start()
        loads.append(l0)
    hload = pltpu.make_async_copy(hidden, hid, lsem.at[0, 1])
    hload.start()
    wload = pltpu.make_async_copy(down, wv, wsem.at[0])
    wload.start()

    f32, bf = jnp.float32, jnp.bfloat16
    ri = routes[...].astype(f32)
    st = scores[...]
    tot = jnp.sum(st, axis=0, keepdims=True)
    low = (st / tot).astype(bf)
    eio = lax.broadcasted_iota(jnp.int32, (64, 128), 0).astype(f32)
    member = jnp.zeros((64, 128), f32)
    score_e = jnp.zeros((64, 128), f32)
    for k in range(8):
        hit = eio == ri[k:k + 1, :]
        member = member + jnp.where(hit, 1.0, 0.0)
        score_e = score_e + jnp.where(hit, st[k:k + 1, :], 0.0)
    before = lax.broadcasted_iota(jnp.int32, (128, 128), 0) < lax.broadcasted_iota(jnp.int32, (128, 128), 1)
    rank = jnp.dot(member.astype(bf), jnp.where(before, 1.0, 0.0).astype(bf), preferred_element_type=f32)
    code_e = jnp.where(member > 0.0, rank, -1.0)
    codes_s[...] = code_e
    score_s[...] = score_e
    code_b = jnp.concatenate([code_e, jnp.full((64, 128), -1.0, f32)], axis=0).astype(bf)
    for p, (A, B, C) in enumerate(ORDERS):
        gb[p][co[B], co[A], :, GB[p] * 128:GB[p] * 128 + 128] = code_b

    def ring(p, axis, slot_of, sems, semr, idx):
        gw = GB[p] * 128 + 128
        half = (gw // 256) * 128
        def cp(i, src_delta, cols, delta):
            ref = slot_of(src_delta)
            if cols is not None:
                ref = ref.at[:, pl.ds(*cols)]
            return rcopy(ref, ref, sems.at[idx + (i,)], semr.at[idx + (i,)], axis, delta)
        return (cp(0, 0, None, 1), cp(1, 0, None, -1), cp(2, -1, (0, half), 1), cp(3, 1, (half, gw - half), -1))

    acp, bcp = [], {}
    for p, (A, B, C) in enumerate(ORDERS):
        acp.append(ring(p, A, lambda d, p=p, A=A, B=B: gb[p].at[co[B], wrap(co[A] + d)], gas, gar, (p,)))
        for k, da in enumerate((0, -1, 1, 2)):
            bcp[p, k] = ring(p, B, lambda d, p=p, A=A, B=B, da=da: gb[p].at[wrap(co[B] + d), wrap(co[A] + da)], gbs, gbr, (p, k))
    pl.semaphore_wait(barrier, 10)
    for p in range(3):
        loads[p].wait()
        go(acp[p][0]); go(acp[p][1])
    for p in range(3):
        go(bcp[p, 0][0]); go(bcp[p, 0][1])

    slots = jnp.concatenate([jnp.sum(jnp.where(eio == ri[k:k + 1, :], rank, 0.0), axis=0, keepdims=True) for k in range(8)], axis=0)
    n8 = lax.broadcasted_iota(jnp.int32, (128, 1024), 1) // 8
    spread = jnp.where(n8 == lax.broadcasted_iota(jnp.int32, (128, 1024), 0), 1.0, 0.0).astype(bf)
    mine = lax.broadcasted_iota(jnp.int32, (8, 1024), 1) % 8 == lax.broadcasted_iota(jnp.int32, (8, 1024), 0)

    def lanes(v):
        return jnp.sum(jnp.where(mine, jnp.dot(v.astype(bf), spread, preferred_element_type=f32), 0.0), axis=0, keepdims=True)
    tgt = CAP * lanes(ri) + lanes(slots)
    wgt = lanes(low)
    hload.wait()

    for p, (A, B, C) in enumerate(ORDERS):
        hw = HB[p] * 128
        r = lax.broadcasted_iota(jnp.int32, (16 * CAP, 1), 0)
        dB = (r >= 4 * CAP).astype(jnp.int32) + (r >= 8 * CAP).astype(jnp.int32) + (r >= 12 * CAP).astype(jnp.int32)
        r1 = r - dB * (4 * CAP)
        dC = (r1 >= CAP).astype(jnp.int32) + (r1 >= 2 * CAP).astype(jnp.int32) + (r1 >= 3 * CAP).astype(jnp.int32)
        slot = r1 - dC * CAP
        base = CAP * (dB * STRIDE[B] + dC * STRIDE[C]) + slot
        for d in (1, 3, 2, 0):
            code = base + CAP * STRIDE[A] * wrap(co[A] + d)
            pick = jnp.where(code.astype(f32) == tgt, wgt, 0.0).astype(jnp.bfloat16)
            rows = jnp.dot(pick, hid[:, hcol[p]:hcol[p] + hw], preferred_element_type=jnp.float32)
            rows = rows.reshape(4, 4, CAP, hw).astype(jnp.bfloat16)
            if d == 0:
                for j in range(4):
                    hb[p][j, co[A]] = rows[j]
            else:
                ha[p][d - 1] = rows
                go(rcopy(ha[p].at[d - 1], hb[p].at[:, co[A]], has.at[p, d - 1], har.at[p, d - 1], A, d))
    hacp = {}
    for p, (A, B, C) in enumerate(ORDERS):
        for d in (1, 2, 3):
            hacp[p, d] = rcopy(ha[p].at[d - 1], hb[p].at[:, wrap(co[A] - d)], has.at[p, d - 1], har.at[p, d - 1], A, d)

    for p in range(3):
        acp[p][0].wait_recv(); go(acp[p][2])
        acp[p][1].wait_recv(); go(acp[p][3])
    for p in range(3):
        for k in (1, 2):
            go(bcp[p, k][0]); go(bcp[p, k][1])
    for p in range(3):
        acp[p][2].wait_recv(); acp[p][3].wait_recv()
        go(bcp[p, 3][0]); go(bcp[p, 3][1])

    j = lax.broadcasted_iota(jnp.int32, (4 * CAP, 1), 0)
    dCj = (j >= CAP).astype(jnp.int32) + (j >= 2 * CAP).astype(jnp.int32) + (j >= 3 * CAP).astype(jnp.int32)
    slotj = (j - dCj * CAP).astype(jnp.float32)
    lane = lax.broadcasted_iota(jnp.int32, (4 * CAP, 64), 1)

    def pack(p, db):
        A, B, C = ORDERS[p]
        gw = GB[p] * 128
        cc = co[C] + dCj
        cc = jnp.where(cc >= 4, cc - 4, cc)
        eid = STRIDE[A] * co[A] + STRIDE[B] * co[B] + STRIDE[C] * cc
        E = jnp.where(lane == eid, 1.0, 0.0).astype(jnp.bfloat16)
        bb = wrap(co[B] + db)

        def one(a, carry):
            codes = jnp.dot(E, gb[p][bb, a, 0:64, gw:gw + 128], preferred_element_type=jnp.float32)
            sel = jnp.where(codes == slotj, 1.0, 0.0).astype(jnp.bfloat16)
            rows = jnp.dot(sel, gb[p][bb, a, :, 0:gw], preferred_element_type=jnp.float32)
            rows = rows.reshape(4, CAP, gw).astype(jnp.bfloat16)
            for dc in range(4):
                sc[p][dc, db % 4, a] = rows[dc]
            return carry
        lax.fori_loop(0, 4, one, 0)
        for dc in (1, 3, 2):
            go(rcopy(sc[p].at[dc, db % 4], fdst(p, bb, 0), gcs.at[p, db % 4, dc - 1], gcr.at[p, db % 4, dc - 1], C, dc))
        cp = pltpu.make_async_copy(sc[p].at[0, db % 4], fdst(p, bb, 0), gcl.at[p, db % 4])
        cp.start()
        locals_[p, db % 4] = cp

    def fdst(p, bb, d):
        A, B, C = ORDERS[p]
        idx = [None, None, None]
        idx[A] = slice(None)
        idx[B] = bb
        idx[C] = wrap(co[C] - d)
        return F.at[idx[0], idx[1], idx[2], :, pl.ds(gcol[p], GB[p] * 128)]

    def hdst(p, bb, d):
        A, B, C = ORDERS[p]
        idx = [None, None, None]
        idx[A] = slice(None)
        idx[B] = bb
        idx[C] = wrap(co[C] - d)
        return HV.at[idx[0], idx[1], idx[2], :, pl.ds(hcol[p], HB[p] * 128)]

    locals_ = {}
    hbcp = {}
    for p, (A, B, C) in enumerate(ORDERS):
        for d in (1, 3, 2):
            hacp[p, d].wait_recv()
        for d in (1, 3, 2):
            hbcp[p, d] = go(rcopy(hb[p].at[wrap(co[B] + d)], hc[p].at[d - 1], hbs.at[p, d - 1], hbr.at[p, d - 1], B, d))
    for p in range(3):
        pack(p, 0)
    for k in range(4):
        for p in range(3):
            bcp[p, k][0].wait_recv(); go(bcp[p, k][2])
            bcp[p, k][1].wait_recv(); go(bcp[p, k][3])

    def hidden_c(p, d):
        A, B, C = ORDERS[p]
        bb = wrap(co[B] - d)
        for dc in (1, 3, 2, 0):
            cs = wrap(co[C] + dc)
            src = hb[p].at[co[B], :, cs] if d == 0 else hc[p].at[d - 1, :, cs]
            if dc == 0:
                dst = hdst(p, bb, 0)
                for a in range(4):
                    dst[a] = src[a]
            else:
                go(rcopy(src, hdst(p, bb, 0), hcs.at[p, d, dc - 1], hcr.at[p, d, dc - 1], C, dc))
    for p in range(3):
        hidden_c(p, 0)
    for p in range(3):
        pack(p, -1)
    for p in range(3):
        pack(p, 1)
    for p in range(3):
        for d in (1, 3, 2):
            hbcp[p, d].wait_recv()
            hidden_c(p, d)
    for p in range(3):
        for k in range(4):
            bcp[p, k][2].wait_recv(); bcp[p, k][3].wait_recv()
        pack(p, 2)
    for p, (A, B, C) in enumerate(ORDERS):
        for d in range(4):
            for dc in (1, 3, 2):
                src = hc[p].at[max(d - 1, 0), :, 0]
                rcopy(src, hdst(p, wrap(co[B] - d), dc), hcs.at[p, d, dc - 1], hcr.at[p, d, dc - 1], C, dc).wait_recv()
    hout = pltpu.make_async_copy(HV, HR, hos.at[0])
    hout.start()
    wload.wait()

    def rest(p):
        return tuple(ax for ax in range(3) if ax != ORDERS[p][1])

    def at_b(ref, p, bb):
        idx = [slice(None)] * 3
        idx[ORDERS[p][1]] = bb
        return ref.at[idx[0], idx[1], idx[2]]

    chunks = [(p, db) for db in (0, -1, 1, 2) for p in range(3)]

    def load(n):
        p, db = chunks[n]
        C = ORDERS[p][2]
        bb = wrap(co[ORDERS[p][1]] + db)
        for dc in (1, 3, 2):
            rcopy(sc[p].at[dc, db % 4], fdst(p, bb, dc), gcs.at[p, db % 4, dc - 1], gcr.at[p, db % 4, dc - 1], C, dc).wait_recv()
        locals_[p, db % 4].wait()
        gw = GB[p] * 128
        cp = pltpu.make_async_copy(at_b(F, p, bb).at[:, :, :, pl.ds(gcol[p], gw)], gch.at[n % 2, :, :, :, pl.ds(0, gw)], gls.at[n % 2])
        cp.start()
        return cp

    def derive(n):
        p, db = chunks[n]
        gw = GB[p] * 128
        B = ORDERS[p][1]
        bb = wrap(co[B] + db)
        R1, R2 = rest(p)
        for i in range(4):
            g2[i * 96:(i + 1) * 96, 0:gw] = gch[n % 2, i, :, :, 0:gw].astype(f32).reshape(96, gw).astype(bf)
        hview = at_b(HV, p, bb)
        acc = jnp.zeros((384, 128), f32)
        for f in range(4):
            proj = lax.dot_general(g2[:, 0:gw], wv[f * 256:(f + 1) * 256, gcol[p]:gcol[p] + gw], (((1,), (1,)), ((), ())),
                                   preferred_element_type=f32)
            q = proj * hview[:, :, :, f * 256:(f + 1) * 256].astype(f32).reshape(384, 256)
            acc = acc + q[:, 0:128] + q[:, 128:256]
        pad = jnp.concatenate([acc.reshape(16, CAP, 128), jnp.zeros((16, 8, 128), f32)], axis=1).reshape(512, 128)
        row = jnp.sum(jnp.transpose(pad), axis=0, keepdims=True)
        for i in range(4):
            ds[p, db % 4, i] = row[:, i * 128:(i + 1) * 128]
        for d1 in range(4):
            for d2 in range(4):
                i = wrap(co[R1] + d1)
                if (db, d1, d2) == (0, 0, 0):
                    dr[p, e] = ds[p, 0, i]
                    continue
                c = [None] * 3
                c[R1], c[R2], c[B] = i, wrap(co[R2] + d2), bb
                pltpu.make_async_remote_copy(src_ref=ds.at[p, db % 4, i], dst_ref=dr.at[p, e], send_sem=dss.at[p], recv_sem=drs.at[p],
                                             device_id={"expert": c[0] * 16 + c[1] * 4 + c[2]}, device_id_type=MESH).start()

    cur = load(0)
    for n in range(12):
        nxt = load(n + 1) if n < 11 else None
        cur.wait()
        derive(n)
        cur = nxt

    home = jnp.zeros((64, 128), f32)
    window = lax.broadcasted_iota(jnp.int32, (64, 128), 1) // 32
    for p in range(3):
        pltpu.make_async_copy(dr.at[p, pl.ds(0, 63)], dr.at[p, pl.ds(0, 63)], drs.at[p]).wait()
        home = home + jnp.where(window == co[rest(p)[1]], dr[p].reshape(64, 128), 0.0)
    home = home + pltpu.roll(home, 64, 1)
    home = home + pltpu.roll(home, 32, 1)
    code_e = codes_s[...]
    score_e = score_s[...]
    rd = jnp.zeros((64, 128), f32)
    for s in range(CAP):
        rd = rd + jnp.where(code_e == float(s), home[:, s:s + 1], 0.0)
    tot = jnp.sum(score_e, axis=0, keepdims=True)
    weight = score_e / tot
    on = code_e >= 0.0
    rd = jnp.where(on, rd / jnp.where(on, weight.astype(bf).astype(f32), 1.0), 0.0)
    center = jnp.sum(weight * rd, axis=0, keepdims=True)
    logit = score_e * (1.0 - score_e) / tot * (rd - center)
    lt = jnp.transpose(logit).astype(bf)
    hcps = []
    for p, (A, B, C) in enumerate(ORDERS):
        gw = GB[p] * 128
        for c0 in range(0, gw, 256):
            add = jnp.dot(lt, router[:, gcol[p] + c0:gcol[p] + c0 + 256], preferred_element_type=f32)
            hnd[:, gcol[p] + c0:gcol[p] + c0 + 256] = (gb[p][co[B], co[A], :, c0:c0 + 256].astype(f32) + add).astype(bf)
        cols = pl.ds(gcol[p], gw)
        cp = pltpu.make_async_remote_copy(src_ref=hnd.at[:, cols], dst_ref=handed.at[:, cols], send_sem=hns.at[p], recv_sem=hnr.at[p],
                                          device_id=other, device_id_type=MESH)
        cp.start()
        hcps.append(cp)
    for p in range(3):
        pltpu.make_async_copy(dr.at[p, pl.ds(0, 63)], dr.at[p, pl.ds(0, 63)], dss.at[p]).wait()
    hout.wait()
    for cp in sends:
        cp.wait_send()
    for cp in hcps:
        cp.wait()


def exchange(routes, scores, router, grad, hidden, down):
    bf, f32 = jnp.bfloat16, jnp.float32
    V = pltpu.VMEM
    D = pltpu.SemaphoreType.DMA
    any_ = pl.BlockSpec(memory_space=pl.ANY)
    vm = pl.BlockSpec(memory_space=pltpu.VMEM)
    gmax = max(GB) * 128
    F, HR, handed = pl.pallas_call(
        comm_kernel,
        out_shape=(jax.ShapeDtypeStruct((4, 4, 4, CAP, 4096), bf), jax.ShapeDtypeStruct((4, 4, 4, CAP, 1024), bf),
                   jax.ShapeDtypeStruct((128, 4096), bf)),
        in_specs=[vm, vm, vm, any_, any_, any_], out_specs=(any_, any_, any_),
        scratch_shapes=[V((1024, 1024), bf), V((4, 4, 4, CAP, 1024), bf), V((1024, 4096), bf), V((2, 4, 4, CAP, gmax), bf),
                        V((384, gmax), bf), V((3, 4, 4, 1, 128), f32), V((3, 64, 1, 128), f32), V((128, 4096), bf),
                        V((64, 128), f32), V((64, 128), f32)]
        + [V((4, 4, 128, g * 128 + 128), bf) for g in GB]
        + [V((4, 4, 4, CAP, g * 128), bf) for g in GB]
        + [V((3, 4, 4, CAP, h * 128), bf) for h in HB]
        + [V((4, 4, 4, CAP, h * 128), bf) for h in HB]
        + [V((3, 4, 4, CAP, h * 128), bf) for h in HB]
        + [D((3, 2)), D((3, 4)), D((3, 4)), D((3, 4, 4)), D((3, 4, 4)), D((3, 4, 3)), D((3, 4, 3)), D((3, 4)),
           D((3, 3)), D((3, 3)), D((3, 3)), D((3, 3)), D((3, 4, 3)), D((3, 4, 3)),
           D((2,)), D((1,)), D((3,)), D((3,)), D((1,)), D((3,)), D((3,))],
        compiler_params=pltpu.CompilerParams(has_side_effects=True, collective_id=0, vmem_limit_bytes=63 * 2**20),
    )(routes, scores, router, grad, hidden, down)
    return F.reshape(64 * CAP, 4096), HR.reshape(64 * CAP, 1024), handed


def body(grad_out, saved_hidden, routes, scores, down_weight, router):
    n_tokens, n_routes, hidden_width = saved_hidden.shape[1:]
    hidden_flat = saved_hidden[0].reshape(n_tokens * n_routes, hidden_width)
    grad_recv, hidden_recv, handed = exchange(routes[0].T, scores[0].T, router[0], grad_out[0], hidden_flat, down_weight[0, 0])
    weight_out = lax.dot_general(hidden_recv, grad_recv, (((0,), (0,)), ((), ())), preferred_element_type=jnp.float32).astype(jnp.bfloat16)
    return weight_out[None, None], handed[None]


def solution(mesh):
    return jax.shard_map(
        body, mesh=mesh,
        in_specs=(P("section", "expert", None), P("section", "expert", None, None), P("section", "expert", None),
                  P("section", "expert", None), P("section", "expert", None, None), P("section", None, None)),
        out_specs=(P("section", "expert", None, None), P("section", "expert", None)), check_vma=False)
```

```python
import functools
import jax
import jax.numpy as jnp
from jax import lax
from jax.experimental import pallas as pl
from jax.experimental.pallas import tpu as pltpu
from jax.sharding import PartitionSpec as P

MESH = pl.DeviceIdType.MESH
CAP = 24
ORDERS = ((0, 1, 2), (1, 2, 0), (2, 0, 1))
STRIDE = (16, 4, 1)
CHUNK = {0: 0, -1: 1, 1: 2, 2: 3}
GB = (10, 12, 10)
HB = (2, 3, 3)


def starts(blocks):
    return tuple(128 * sum(blocks[:i]) for i in range(len(blocks)))


def comm_kernel(routes, scores, router, grad, hidden, down, F, HT, part, handed, hid, HV, wv, gch, g2, acc_s, stage, U0, U1, U2, lv0, lv1, lv2, ds, dr, hnd, codes_s, score_s,
                gb0, gb1, gb2, sc0, sc1, sc2, ha0, ha1, ha2, hb0, hb1, hb2, hc0, hc1, hc2,
                lsem, gas, gar, gbs, gbr, gcs, gcr, gcl, has, har, hbs, hbr, hcs, hcr, gls, wsem, dss, drs, hos, pos, lvs, hns, hnr):
    gb, sc, ha, hb, hc = (gb0, gb1, gb2), (sc0, sc1, sc2), (ha0, ha1, ha2), (hb0, hb1, hb2), (hc0, hc1, hc2)
    e = lax.axis_index("expert")
    co = (e // 16, (e // 4) % 4, e % 4)
    gcol, hcol = starts(GB), starts(HB)
    U, lv = (U0, U1, U2), (lv0, lv1, lv2)

    def wrap(v):
        return lax.rem(v + 4, 4)

    def peer(axis, delta):
        c = list(co)
        c[axis] = wrap(co[axis] + delta)
        return {"expert": c[0] * 16 + c[1] * 4 + c[2]}

    def rcopy(src, dst, ss, rs, axis, delta):
        return pltpu.make_async_remote_copy(src_ref=src, dst_ref=dst, send_sem=ss, recv_sem=rs,
                                            device_id=peer(axis, delta), device_id_type=MESH)

    other = {"section": 1 - lax.axis_index("section")}
    barrier = pltpu.get_barrier_semaphore()
    for axis in range(3):
        for d in (1, 2, 3):
            pl.semaphore_signal(barrier, inc=1, device_id=peer(axis, d), device_id_type=MESH)
    pl.semaphore_signal(barrier, inc=1, device_id=other, device_id_type=MESH)

    sends = []

    def go(cp):
        cp.start()
        sends.append(cp)
        return cp

    loads = []
    for p, (A, B, C) in enumerate(ORDERS):
        gw = GB[p] * 128
        own = gb[p].at[co[B], co[A]]
        l0 = pltpu.make_async_copy(grad.at[:, pl.ds(gcol[p], gw)], own.at[:, pl.ds(0, gw)], lsem.at[p, 0])
        l0.start()
        loads.append(l0)
    hload = pltpu.make_async_copy(hidden, hid, lsem.at[0, 1])
    hload.start()
    wload = pltpu.make_async_copy(down, wv, wsem.at[0])
    wload.start()

    f32, bf = jnp.float32, jnp.bfloat16
    ri = routes[...].astype(f32)
    st = scores[...]
    tot = jnp.sum(st, axis=0, keepdims=True)
    low = (st / tot).astype(bf)
    eio = lax.broadcasted_iota(jnp.int32, (64, 128), 0).astype(f32)
    member = jnp.zeros((64, 128), f32)
    score_e = jnp.zeros((64, 128), f32)
    for k in range(8):
        hit = eio == ri[k:k + 1, :]
        member = member + jnp.where(hit, 1.0, 0.0)
        score_e = score_e + jnp.where(hit, st[k:k + 1, :], 0.0)
    before = lax.broadcasted_iota(jnp.int32, (128, 128), 0) < lax.broadcasted_iota(jnp.int32, (128, 128), 1)
    rank = jnp.dot(member.astype(bf), jnp.where(before, 1.0, 0.0).astype(bf), preferred_element_type=f32)
    code_e = jnp.where(member > 0.0, rank, -1.0)
    codes_s[...] = code_e
    score_s[...] = score_e
    code_b = jnp.concatenate([code_e, jnp.full((64, 128), -1.0, f32)], axis=0).astype(bf)
    for p, (A, B, C) in enumerate(ORDERS):
        gb[p][co[B], co[A], :, GB[p] * 128:GB[p] * 128 + 128] = code_b

    def ring(p, axis, slot_of, sems, semr, idx):
        gw = GB[p] * 128 + 128
        half = (gw // 256) * 128
        def cp(i, src_delta, cols, delta):
            ref = slot_of(src_delta)
            if cols is not None:
                ref = ref.at[:, pl.ds(*cols)]
            return rcopy(ref, ref, sems.at[idx + (i,)], semr.at[idx + (i,)], axis, delta)
        return (cp(0, 0, None, 1), cp(1, 0, None, -1), cp(2, -1, (0, half), 1), cp(3, 1, (half, gw - half), -1))

    acp, bcp = [], {}
    for p, (A, B, C) in enumerate(ORDERS):
        acp.append(ring(p, A, lambda d, p=p, A=A, B=B: gb[p].at[co[B], wrap(co[A] + d)], gas, gar, (p,)))
        for k, da in enumerate((0, -1, 1, 2)):
            bcp[p, k] = ring(p, B, lambda d, p=p, A=A, B=B, da=da: gb[p].at[wrap(co[B] + d), wrap(co[A] + da)], gbs, gbr, (p, k))
    pl.semaphore_wait(barrier, 10)
    for p in range(3):
        loads[p].wait()
        go(acp[p][0]); go(acp[p][1])
    for p in range(3):
        go(bcp[p, 0][0]); go(bcp[p, 0][1])

    slots = jnp.concatenate([jnp.sum(jnp.where(eio == ri[k:k + 1, :], rank, 0.0), axis=0, keepdims=True) for k in range(8)], axis=0)
    n8 = lax.broadcasted_iota(jnp.int32, (128, 1024), 1) // 8
    spread = jnp.where(n8 == lax.broadcasted_iota(jnp.int32, (128, 1024), 0), 1.0, 0.0).astype(bf)
    mine = lax.broadcasted_iota(jnp.int32, (8, 1024), 1) % 8 == lax.broadcasted_iota(jnp.int32, (8, 1024), 0)

    def lanes(v):
        return jnp.sum(jnp.where(mine, jnp.dot(v.astype(bf), spread, preferred_element_type=f32), 0.0), axis=0, keepdims=True)
    tgt = CAP * lanes(ri) + lanes(slots)
    wgt = lanes(low)
    hload.wait()

    for p, (A, B, C) in enumerate(ORDERS):
        hw = HB[p] * 128
        r = lax.broadcasted_iota(jnp.int32, (16 * CAP, 1), 0)
        dB = (r >= 4 * CAP).astype(jnp.int32) + (r >= 8 * CAP).astype(jnp.int32) + (r >= 12 * CAP).astype(jnp.int32)
        r1 = r - dB * (4 * CAP)
        dC = (r1 >= CAP).astype(jnp.int32) + (r1 >= 2 * CAP).astype(jnp.int32) + (r1 >= 3 * CAP).astype(jnp.int32)
        slot = r1 - dC * CAP
        base = CAP * (dB * STRIDE[B] + dC * STRIDE[C]) + slot
        for d in (1, 3, 2, 0):
            code = base + CAP * STRIDE[A] * wrap(co[A] + d)
            pick = jnp.where(code.astype(f32) == tgt, wgt, 0.0).astype(jnp.bfloat16)
            rows = jnp.dot(pick, hid[:, hcol[p]:hcol[p] + hw], preferred_element_type=jnp.float32)
            rows = rows.reshape(4, 4, CAP, hw).astype(jnp.bfloat16)
            if d == 0:
                for j in range(4):
                    hb[p][j, co[A]] = rows[j]
            else:
                ha[p][d - 1] = rows
                go(rcopy(ha[p].at[d - 1], hb[p].at[:, co[A]], has.at[p, d - 1], har.at[p, d - 1], A, d))
    hacp = {}
    for p, (A, B, C) in enumerate(ORDERS):
        for d in (1, 2, 3):
            hacp[p, d] = rcopy(ha[p].at[d - 1], hb[p].at[:, wrap(co[A] - d)], has.at[p, d - 1], har.at[p, d - 1], A, d)

    for p in range(3):
        acp[p][0].wait_recv(); go(acp[p][2])
        acp[p][1].wait_recv(); go(acp[p][3])
    for p in range(3):
        for k in (1, 2):
            go(bcp[p, k][0]); go(bcp[p, k][1])
    for p in range(3):
        acp[p][2].wait_recv(); acp[p][3].wait_recv()
        go(bcp[p, 3][0]); go(bcp[p, 3][1])

    j = lax.broadcasted_iota(jnp.int32, (4 * CAP, 1), 0)
    dCj = (j >= CAP).astype(jnp.int32) + (j >= 2 * CAP).astype(jnp.int32) + (j >= 3 * CAP).astype(jnp.int32)
    slotj = (j - dCj * CAP).astype(jnp.float32)
    lane = lax.broadcasted_iota(jnp.int32, (4 * CAP, 64), 1)

    def pack(p, db):
        A, B, C = ORDERS[p]
        gw = GB[p] * 128
        cc = co[C] + dCj
        cc = jnp.where(cc >= 4, cc - 4, cc)
        eid = STRIDE[A] * co[A] + STRIDE[B] * co[B] + STRIDE[C] * cc
        E = jnp.where(lane == eid, 1.0, 0.0).astype(jnp.bfloat16)
        bb = wrap(co[B] + db)

        def one(a, carry):
            codes = jnp.dot(E, gb[p][bb, a, 0:64, gw:gw + 128], preferred_element_type=jnp.float32)
            sel = jnp.where(codes == slotj, 1.0, 0.0).astype(jnp.bfloat16)
            rows = jnp.dot(sel, gb[p][bb, a, :, 0:gw], preferred_element_type=jnp.float32)
            rows = rows.reshape(4, CAP, gw).astype(jnp.bfloat16)
            for dc in range(4):
                if db == 2 and dc == 0:
                    if A < C:
                        lv[p][a, co[C]] = rows[0]
                    else:
                        lv[p][co[C], a] = rows[0]
                else:
                    sc[p][dc, n % 3, a] = rows[dc]
            return carry
        n = CHUNK[db]
        if db == 2:
            for cp in csends[p]:
                cp.wait_send()
            locals_[p, 0].wait()
        lax.fori_loop(0, 4, one, 0)
        for dc in (1, 3, 2):
            cp = rcopy(sc[p].at[dc, n % 3], fdst(p, db, 0), gcs.at[p, n, dc - 1], gcr.at[p, n, dc - 1], C, dc)
            cp.start()
            (csends[p] if db == 0 else sends).append(cp)
        if db != 2:
            cp = pltpu.make_async_copy(sc[p].at[0, n % 3], fdst(p, db, 0), gcl.at[p, n])
            cp.start()
            locals_[p, n] = cp

    csends = ([], [], [])

    def fdst(p, db, d):
        A, B, C = ORDERS[p]
        c = wrap(co[C] - d)
        if db == 2:
            return lv[p].at[:, c] if A < C else lv[p].at[c, :]
        cols = pl.ds(gcol[p], GB[p] * 128)
        return F.at[CHUNK[db], :, c, :, cols] if A < C else F.at[CHUNK[db], c, :, :, cols]

    def hdst(p, bb, d):
        A, B, C = ORDERS[p]
        idx = [None, None, None]
        idx[A] = slice(None)
        idx[B] = bb
        idx[C] = wrap(co[C] - d)
        return HV.at[idx[0], idx[1], idx[2], :, pl.ds(hcol[p], HB[p] * 128)]

    locals_ = {}
    hbcp = {}
    for p, (A, B, C) in enumerate(ORDERS):
        for d in (1, 3, 2):
            hacp[p, d].wait_recv()
        for d in (1, 3, 2):
            hbcp[p, d] = go(rcopy(hb[p].at[wrap(co[B] + d)], hc[p].at[d - 1], hbs.at[p, d - 1], hbr.at[p, d - 1], B, d))
    for p in range(3):
        pack(p, 0)
    for k in range(4):
        for p in range(3):
            bcp[p, k][0].wait_recv(); go(bcp[p, k][2])
            bcp[p, k][1].wait_recv(); go(bcp[p, k][3])

    def hidden_c(p, d):
        A, B, C = ORDERS[p]
        bb = wrap(co[B] - d)
        for dc in (1, 3, 2, 0):
            cs = wrap(co[C] + dc)
            src = hb[p].at[co[B], :, cs] if d == 0 else hc[p].at[d - 1, :, cs]
            if dc == 0:
                dst = hdst(p, bb, 0)
                for a in range(4):
                    dst[a] = src[a]
            else:
                go(rcopy(src, hdst(p, bb, 0), hcs.at[p, d, dc - 1], hcr.at[p, d, dc - 1], C, dc))
    for p in range(3):
        hidden_c(p, 0)
    for p in range(3):
        pack(p, -1)
    for p in range(3):
        pack(p, 1)
    for p in range(3):
        for d in (1, 3, 2):
            hbcp[p, d].wait_recv()
            hidden_c(p, d)
    for p in range(3):
        for k in range(4):
            bcp[p, k][2].wait_recv(); bcp[p, k][3].wait_recv()
        pack(p, 2)
    for p, (A, B, C) in enumerate(ORDERS):
        for d in range(4):
            for dc in (1, 3, 2):
                src = hc[p].at[max(d - 1, 0), :, 0]
                rcopy(src, hdst(p, wrap(co[B] - d), dc), hcs.at[p, d, dc - 1], hcr.at[p, d, dc - 1], C, dc).wait_recv()
    wload.wait()

    def rest(p):
        return tuple(ax for ax in range(3) if ax != ORDERS[p][1])

    def hview(p, db):
        idx = [slice(None)] * 3
        idx[ORDERS[p][1]] = wrap(co[ORDERS[p][1]] + db)
        return HV.at[idx[0], idx[1], idx[2]]

    def turn(p, db, off):
        view = hview(p, db)

        def one(j, carry):
            v = view[:, :, :, pl.ds(pl.multiple_of(j * 128, 128), 128)].astype(f32).reshape(384, 128)
            hid[pl.ds(pl.multiple_of(j * 128, 128), 128), off:off + 384] = jnp.transpose(v).astype(bf)
            return carry
        lax.fori_loop(0, 8, one, 0)

    for p in range(3):
        gw = GB[p] * 128
        turn(p, 1, 0)
        turn(p, 2, 384)
        cp = pltpu.make_async_copy(hid.at[:, pl.ds(0, 768)], HT.at[p], hos.at[0])
        cp.start()
        view = hview(p, 2)
        for i in range(4):
            g2[i * 96:(i + 1) * 96, 0:1024] = view[i].astype(f32).reshape(96, 1024).astype(bf)

        def prod(ct, carry, p=p):
            cols = pl.ds(pl.multiple_of(ct * 256, 256), 256)
            wcols = pl.ds(pl.multiple_of(gcol[p] + ct * 256, 256), 256)
            u = jnp.dot(g2[0:384, 0:1024], wv[:, wcols], preferred_element_type=f32)
            U[p][:, :, :, cols] = u.reshape(4, 4, CAP, 256).astype(bf)
            return carry
        lax.fori_loop(0, gw // 256, prod, 0)
        cp.wait()

    def arrived(p, db):
        C, n = ORDERS[p][2], CHUNK[db]
        for dc in (1, 3, 2):
            rcopy(sc[p].at[dc, n % 3], fdst(p, db, dc), gcs.at[p, n, dc - 1], gcr.at[p, n, dc - 1], C, dc).wait_recv()
        if n in (1, 2):
            locals_[p, n].wait()

    def load(p, db, slot):
        gw = GB[p] * 128
        arrived(p, db)
        cp = pltpu.make_async_copy(F.at[CHUNK[db], :, :, :, pl.ds(gcol[p], gw)], gch.at[slot, :, :, :, pl.ds(0, gw)], gls.at[slot])
        cp.start()
        return cp

    def relay(p, slot, r0):
        gw = GB[p] * 128
        for i in range(4):
            g2[r0 + i * 96:r0 + (i + 1) * 96, 0:gw] = gch[slot, i, :, :, 0:gw].astype(f32).reshape(96, gw).astype(bf)

    def derive(p, dbs):
        gw = GB[p] * 128
        m = 384 * len(dbs)

        def one(f, carry):
            rows = pl.ds(pl.multiple_of(f * 256, 256), 256)
            proj = lax.dot_general(g2[0:m, 0:gw], wv[rows, gcol[p]:gcol[p] + gw], (((1,), (1,)), ((), ())),
                                   preferred_element_type=f32)
            for k, db in enumerate(dbs):
                h = hview(p, db)[:, :, :, rows].astype(f32).reshape(384, 256)
                q = proj[k * 384:(k + 1) * 384] * h
                acc_s[k * 384:(k + 1) * 384, :] = jnp.where(f > 0, acc_s[k * 384:(k + 1) * 384, :], 0.0) + q[:, 0:128] + q[:, 128:256]
            return carry
        lax.fori_loop(0, 4, one, 0)
        for k, db in enumerate(dbs):
            give(p, db, acc_s[k * 384:(k + 1) * 384, :])

    def give(p, db, acc):
        B = ORDERS[p][1]
        bb = wrap(co[B] + db)
        R1, R2 = rest(p)
        pad = jnp.concatenate([acc.reshape(16, CAP, 128), jnp.zeros((16, 8, 128), f32)], axis=1).reshape(512, 128)
        row = jnp.sum(jnp.transpose(pad), axis=0, keepdims=True)
        for i in range(4):
            ds[p, db % 4, i] = row[:, i * 128:(i + 1) * 128]
        for d1 in range(4):
            for d2 in range(4):
                i = wrap(co[R1] + d1)
                if (db, d1, d2) == (0, 0, 0):
                    dr[p, e] = ds[p, 0, i]
                    continue
                c = [None] * 3
                c[R1], c[R2], c[B] = i, wrap(co[R2] + d2), bb
                pltpu.make_async_remote_copy(src_ref=ds.at[p, db % 4, i], dst_ref=dr.at[p, e], send_sem=dss.at[p], recv_sem=drs.at[p],
                                             device_id={"expert": c[0] * 16 + c[1] * 4 + c[2]}, device_id_type=MESH).start()

    def gradient(p):
        gw = GB[p] * 128

        def out(ct, slot):
            cols = pl.ds(pl.multiple_of(gcol[p] + ct * 256, 256), 256)
            return pltpu.make_async_copy(stage.at[slot], part.at[:, cols], pos.at[slot])

        def one(ct, carry):
            slot = lax.rem(ct, 2)

            @pl.when(ct >= 2)
            def _():
                out(ct - 2, slot).wait()
            stage[slot] = jnp.dot(hid[:, 0:768], g2[:, pl.ds(pl.multiple_of(ct * 256, 256), 256)], preferred_element_type=f32).astype(bf)
            out(ct, slot).start()
            return carry
        n = gw // 256
        lax.fori_loop(0, n, one, 0)
        out(n - 2, (n - 2) % 2).wait()
        out(n - 1, (n - 1) % 2).wait()

    cur = (load(0, 0, 0), load(0, -1, 1))
    for p in range(3):
        turn(p, 0, 0)
        turn(p, -1, 384)
        cur[0].wait(); relay(p, 0, 0)
        cur[1].wait(); relay(p, 1, 384)
        if p < 2:
            cur = (load(p + 1, 0, 0), load(p + 1, -1, 1))
        derive(p, (0, -1))
        gradient(p)
    cur = load(0, 1, 0)
    for p in range(3):
        cur.wait(); relay(p, p % 2, 0)
        if p < 2:
            cur = load(p + 1, 1, (p + 1) % 2)
        derive(p, (1,))
    lcps = []
    for p in range(3):
        gw = GB[p] * 128
        arrived(p, 2)
        cp = pltpu.make_async_copy(lv[p], F.at[3, :, :, :, pl.ds(gcol[p], gw)], lvs.at[p])
        cp.start()
        lcps.append(cp)

        def one(ij, carry, p=p):
            i, j = ij // 4, lax.rem(ij, 4)
            t = jnp.zeros((CAP, 128), f32)
            for k in range(GB[p]):
                t = t + U[p][i, j, :, k * 128:(k + 1) * 128].astype(f32) * lv[p][i, j, :, k * 128:(k + 1) * 128].astype(f32)
            acc_s[pl.ds(pl.multiple_of(ij * CAP, 8), CAP), :] = t
            return carry
        lax.fori_loop(0, 16, one, 0)
        give(p, 2, acc_s[0:384, :])

    home = jnp.zeros((64, 128), f32)
    window = lax.broadcasted_iota(jnp.int32, (64, 128), 1) // 32
    for p in range(3):
        pltpu.make_async_copy(dr.at[p, pl.ds(0, 63)], dr.at[p, pl.ds(0, 63)], drs.at[p]).wait()
        home = home + jnp.where(window == co[rest(p)[1]], dr[p].reshape(64, 128), 0.0)
    home = home + pltpu.roll(home, 64, 1)
    home = home + pltpu.roll(home, 32, 1)
    code_e = codes_s[...]
    score_e = score_s[...]
    rd = jnp.zeros((64, 128), f32)
    for s in range(CAP):
        rd = rd + jnp.where(code_e == float(s), home[:, s:s + 1], 0.0)
    tot = jnp.sum(score_e, axis=0, keepdims=True)
    weight = score_e / tot
    on = code_e >= 0.0
    rd = jnp.where(on, rd / jnp.where(on, weight.astype(bf).astype(f32), 1.0), 0.0)
    center = jnp.sum(weight * rd, axis=0, keepdims=True)
    logit = score_e * (1.0 - score_e) / tot * (rd - center)
    lt = jnp.transpose(logit).astype(bf)
    hcps = []
    for p, (A, B, C) in enumerate(ORDERS):
        gw = GB[p] * 128
        for c0 in range(0, gw, 256):
            add = jnp.dot(lt, router[:, gcol[p] + c0:gcol[p] + c0 + 256], preferred_element_type=f32)
            hnd[:, gcol[p] + c0:gcol[p] + c0 + 256] = (gb[p][co[B], co[A], :, c0:c0 + 256].astype(f32) + add).astype(bf)
        cols = pl.ds(gcol[p], gw)
        cp = pltpu.make_async_remote_copy(src_ref=hnd.at[:, cols], dst_ref=handed.at[:, cols], send_sem=hns.at[p], recv_sem=hnr.at[p],
                                          device_id=other, device_id_type=MESH)
        cp.start()
        hcps.append(cp)
    for p in range(3):
        pltpu.make_async_copy(dr.at[p, pl.ds(0, 63)], dr.at[p, pl.ds(0, 63)], dss.at[p]).wait()
    for cp in lcps:
        cp.wait()
    for cp in sends:
        cp.wait_send()
    for cp in hcps:
        cp.wait()


def exchange(routes, scores, router, grad, hidden, down):
    bf, f32 = jnp.bfloat16, jnp.float32
    V = pltpu.VMEM
    D = pltpu.SemaphoreType.DMA
    any_ = pl.BlockSpec(memory_space=pl.ANY)
    vm = pl.BlockSpec(memory_space=pltpu.VMEM)
    gmax = max(GB) * 128
    F, HT, part, handed = pl.pallas_call(
        comm_kernel,
        out_shape=(jax.ShapeDtypeStruct((4, 4, 4, CAP, 4096), bf), jax.ShapeDtypeStruct((3, 1024, 768), bf),
                   jax.ShapeDtypeStruct((1024, 4096), bf), jax.ShapeDtypeStruct((128, 4096), bf)),
        in_specs=[vm, vm, vm, any_, any_, any_], out_specs=(any_, any_, any_, any_),
        scratch_shapes=[V((1024, 1024), bf), V((4, 4, 4, CAP, 1024), bf), V((1024, 4096), bf), V((2, 4, 4, CAP, gmax), bf),
                        V((768, gmax), bf), V((768, 128), f32), V((2, 1024, 256), bf)]
        + [V((4, 4, CAP, g * 128), bf) for g in GB] * 2
        + [V((3, 4, 4, 1, 128), f32), V((3, 64, 1, 128), f32), V((128, 4096), bf),
                        V((64, 128), f32), V((64, 128), f32)]
        + [V((4, 4, 128, g * 128 + 128), bf) for g in GB]
        + [V((4, 3, 4, CAP, g * 128), bf) for g in GB]
        + [V((3, 4, 4, CAP, h * 128), bf) for h in HB]
        + [V((4, 4, 4, CAP, h * 128), bf) for h in HB]
        + [V((3, 4, 4, CAP, h * 128), bf) for h in HB]
        + [D((3, 2)), D((3, 4)), D((3, 4)), D((3, 4, 4)), D((3, 4, 4)), D((3, 4, 3)), D((3, 4, 3)), D((3, 4)),
           D((3, 3)), D((3, 3)), D((3, 3)), D((3, 3)), D((3, 4, 3)), D((3, 4, 3)),
           D((2,)), D((1,)), D((3,)), D((3,)), D((1,)), D((2,)), D((3,)), D((3,)), D((3,))],
        compiler_params=pltpu.CompilerParams(has_side_effects=True, collective_id=0, vmem_limit_bytes=67043328),
    )(routes, scores, router, grad, hidden, down)
    return F.reshape(64 * CAP, 4096), HT, part, handed


def finish_kernel(part, turned, rows, out):
    more = jnp.dot(turned[0], rows[...], preferred_element_type=jnp.float32)
    out[...] = (part[...].astype(jnp.float32) + more).astype(jnp.bfloat16)


def finish(rows, turned, part):
    edges = [sum(GB[:i]) // 2 for i in (1, 2)]
    return pl.pallas_call(
        finish_kernel,
        out_shape=jax.ShapeDtypeStruct((1024, 4096), jnp.bfloat16),
        grid=(16,),
        in_specs=[pl.BlockSpec((1024, 256), lambda i: (0, i)),
                  pl.BlockSpec((1, 1024, 768), lambda i: ((i >= edges[0]).astype(jnp.int32) + (i >= edges[1]).astype(jnp.int32), 0, 0)),
                  pl.BlockSpec((768, 256), lambda i: (1, i))],
        out_specs=pl.BlockSpec((1024, 256), lambda i: (0, i)),
        compiler_params=pltpu.CompilerParams(dimension_semantics=("arbitrary",), vmem_limit_bytes=40 * 2**20),
    )(part, turned, rows)


def body(grad_out, saved_hidden, routes, scores, down_weight, router):
    n_tokens, n_routes, hidden_width = saved_hidden.shape[1:]
    hidden_flat = saved_hidden[0].reshape(n_tokens * n_routes, hidden_width)
    rows, turned, part, handed = exchange(routes[0].T, scores[0].T, router[0], grad_out[0], hidden_flat, down_weight[0, 0])
    weight_out = finish(rows, turned, part)
    return weight_out[None, None], handed[None]


def solution(mesh):
    return jax.shard_map(
        body, mesh=mesh,
        in_specs=(P("section", "expert", None), P("section", "expert", None, None), P("section", "expert", None),
                  P("section", "expert", None), P("section", "expert", None, None), P("section", None, None)),
        out_specs=(P("section", "expert", None, None), P("section", "expert", None)), check_vma=False)
```

```python
import functools
import jax
import jax.numpy as jnp
from jax import lax
from jax.experimental import pallas as pl
from jax.experimental.pallas import tpu as pltpu
from jax.sharding import PartitionSpec as P

MESH = pl.DeviceIdType.MESH
CAP = 24
ORDERS = ((0, 1, 2), (1, 2, 0), (2, 0, 1))
STRIDE = (16, 4, 1)
GB = (10, 12, 10)
HB = (2, 3, 3)


def starts(blocks):
    return tuple(128 * sum(blocks[:i]) for i in range(len(blocks)))


def comm_kernel(routes, scores, router, grad, hidden, down, F, HR, handed, hid, HV, wv, gch, g2, ds, dr, hnd, codes_s, score_s, tab, rc, U0, U1, U2, lv0, lv1, lv2,
                gb0, gb1, gb2, sc0, sc1, sc2, ha0, ha1, ha2, hb0, hb1, hb2, hc0, hc1, hc2,
                lsem, gas, gar, gbs, gbr, gcs, gcr, gcl, has, har, hbs, hbr, hcs, hcr, gls, wsem, dss, drs, hos, lvs, tss, trs):
    gb, sc, ha, hb, hc = (gb0, gb1, gb2), (sc0, sc1, sc2), (ha0, ha1, ha2), (hb0, hb1, hb2), (hc0, hc1, hc2)
    e = lax.axis_index("expert")
    co = (e // 16, (e // 4) % 4, e % 4)
    gcol, hcol = starts(GB), starts(HB)
    U, lv = (U0, U1, U2), (lv0, lv1, lv2)

    def wrap(v):
        return lax.rem(v + 4, 4)

    def peer(axis, delta):
        c = list(co)
        c[axis] = wrap(co[axis] + delta)
        return {"expert": c[0] * 16 + c[1] * 4 + c[2]}

    def rcopy(src, dst, ss, rs, axis, delta):
        return pltpu.make_async_remote_copy(src_ref=src, dst_ref=dst, send_sem=ss, recv_sem=rs,
                                            device_id=peer(axis, delta), device_id_type=MESH)

    def plane(p, da, db):
        A, B, C = ORDERS[p]
        c = list(co)
        c[A], c[B] = wrap(co[A] + da), wrap(co[B] + db)
        return c, {"expert": c[0] * 16 + c[1] * 4 + c[2]}

    barrier = pltpu.get_barrier_semaphore()
    for axis in range(3):
        for d in (1, 2, 3):
            pl.semaphore_signal(barrier, inc=1, device_id=peer(axis, d), device_id_type=MESH)
    for p in range(3):
        for da in (1, 2, 3):
            for db in (1, 2, 3):
                pl.semaphore_signal(barrier, inc=1, device_id=plane(p, da, db)[1], device_id_type=MESH)

    sends = []

    def go(cp):
        cp.start()
        sends.append(cp)
        return cp

    loads = []
    for p, (A, B, C) in enumerate(ORDERS):
        gw = GB[p] * 128
        own = gb[p].at[co[B], co[A]]
        l0 = pltpu.make_async_copy(grad.at[:, pl.ds(gcol[p], gw)], own.at[:, pl.ds(0, gw)], lsem.at[p, 0])
        l0.start()
        loads.append(l0)
    hload = pltpu.make_async_copy(hidden, hid, lsem.at[0, 1])
    hload.start()
    wload = pltpu.make_async_copy(down, wv, wsem.at[0])
    wload.start()

    def ring(p, axis, slot_of, sems, semr, idx):
        gw = GB[p] * 128
        half = (gw // 256) * 128
        def cp(i, src_delta, cols, delta):
            ref = slot_of(src_delta)
            if cols is not None:
                ref = ref.at[:, pl.ds(*cols)]
            return rcopy(ref, ref, sems.at[idx + (i,)], semr.at[idx + (i,)], axis, delta)
        return (cp(0, 0, None, 1), cp(1, 0, None, -1), cp(2, -1, (0, half), 1), cp(3, 1, (half, gw - half), -1))

    acp, bcp = [], {}
    for p, (A, B, C) in enumerate(ORDERS):
        acp.append(ring(p, A, lambda d, p=p, A=A, B=B: gb[p].at[co[B], wrap(co[A] + d)], gas, gar, (p,)))
        for k, da in enumerate((0, -1, 1, 2)):
            bcp[p, k] = ring(p, B, lambda d, p=p, A=A, B=B, da=da: gb[p].at[wrap(co[B] + d), wrap(co[A] + da)], gbs, gbr, (p, k))
    pl.semaphore_wait(barrier, 36)
    for p in range(3):
        loads[p].wait()
        go(acp[p][0]); go(acp[p][1])
    for p in range(3):
        go(bcp[p, 0][0]); go(bcp[p, 0][1])

    f32, bf = jnp.float32, jnp.bfloat16
    ri = routes[...].astype(f32)
    st = scores[...]
    tot = jnp.sum(st, axis=0, keepdims=True)
    low = (st / tot).astype(bf)
    eio = lax.broadcasted_iota(jnp.int32, (64, 128), 0).astype(f32)
    member = jnp.zeros((64, 128), f32)
    score_e = jnp.zeros((64, 128), f32)
    for k in range(8):
        hit = eio == ri[k:k + 1, :]
        member = member + jnp.where(hit, 1.0, 0.0)
        score_e = score_e + jnp.where(hit, st[k:k + 1, :], 0.0)
    before = lax.broadcasted_iota(jnp.int32, (128, 128), 0) < lax.broadcasted_iota(jnp.int32, (128, 128), 1)
    rank = jnp.dot(member.astype(bf), jnp.where(before, 1.0, 0.0).astype(bf), preferred_element_type=f32)
    code_e = jnp.where(member > 0.0, rank, -1.0)
    codes_s[...] = code_e
    score_s[...] = score_e
    for k in range(64):
        tab[k // 16, (k // 4) % 4, k % 4] = code_e[k:k + 1, :]

    for p, (A, B, C) in enumerate(ORDERS):
        for da in range(4):
            for db in range(4):
                c, dev = plane(p, da, db)
                idx = list(c)
                if da == 0 and db == 0:
                    for k in range(4):
                        idx[C] = k
                        rc[p, co[B] * 4 + co[A], k] = tab[idx[0], idx[1], idx[2]]
                    continue
                idx[C] = slice(None)
                pltpu.make_async_remote_copy(src_ref=tab.at[idx[0], idx[1], idx[2]], dst_ref=rc.at[p, co[B] * 4 + co[A]],
                                             send_sem=tss.at[p], recv_sem=trs.at[p], device_id=dev, device_id_type=MESH).start()

    slots = jnp.concatenate([jnp.sum(jnp.where(eio == ri[k:k + 1, :], rank, 0.0), axis=0, keepdims=True) for k in range(8)], axis=0)
    n8 = lax.broadcasted_iota(jnp.int32, (128, 1024), 1) // 8
    spread = jnp.where(n8 == lax.broadcasted_iota(jnp.int32, (128, 1024), 0), 1.0, 0.0).astype(bf)
    mine = lax.broadcasted_iota(jnp.int32, (8, 1024), 1) % 8 == lax.broadcasted_iota(jnp.int32, (8, 1024), 0)

    def lanes(v):
        return jnp.sum(jnp.where(mine, jnp.dot(v.astype(bf), spread, preferred_element_type=f32), 0.0), axis=0, keepdims=True)
    tgt = CAP * lanes(ri) + lanes(slots)
    wgt = lanes(low)
    hload.wait()

    for p, (A, B, C) in enumerate(ORDERS):
        hw = HB[p] * 128
        r = lax.broadcasted_iota(jnp.int32, (16 * CAP, 1), 0)
        dB = (r >= 4 * CAP).astype(jnp.int32) + (r >= 8 * CAP).astype(jnp.int32) + (r >= 12 * CAP).astype(jnp.int32)
        r1 = r - dB * (4 * CAP)
        dC = (r1 >= CAP).astype(jnp.int32) + (r1 >= 2 * CAP).astype(jnp.int32) + (r1 >= 3 * CAP).astype(jnp.int32)
        slot = r1 - dC * CAP
        base = CAP * (dB * STRIDE[B] + dC * STRIDE[C]) + slot
        for d in (1, 3, 2, 0):
            code = base + CAP * STRIDE[A] * wrap(co[A] + d)
            pick = jnp.where(code.astype(f32) == tgt, wgt, 0.0).astype(jnp.bfloat16)
            rows = jnp.dot(pick, hid[:, hcol[p]:hcol[p] + hw], preferred_element_type=jnp.float32)
            rows = rows.reshape(4, 4, CAP, hw).astype(jnp.bfloat16)
            if d == 0:
                for j in range(4):
                    hb[p][j, co[A]] = rows[j]
            else:
                ha[p][d - 1] = rows
                go(rcopy(ha[p].at[d - 1], hb[p].at[:, co[A]], has.at[p, d - 1], har.at[p, d - 1], A, d))
    hacp = {}
    for p, (A, B, C) in enumerate(ORDERS):
        for d in (1, 2, 3):
            hacp[p, d] = rcopy(ha[p].at[d - 1], hb[p].at[:, wrap(co[A] - d)], has.at[p, d - 1], har.at[p, d - 1], A, d)

    for p in range(3):
        acp[p][0].wait_recv(); go(acp[p][2])
        acp[p][1].wait_recv(); go(acp[p][3])
    for p in range(3):
        for k in (1, 2):
            go(bcp[p, k][0]); go(bcp[p, k][1])
    for p in range(3):
        acp[p][2].wait_recv(); acp[p][3].wait_recv()
        go(bcp[p, 3][0]); go(bcp[p, 3][1])

    j = lax.broadcasted_iota(jnp.int32, (4 * CAP, 1), 0)
    dCj = (j >= CAP).astype(jnp.int32) + (j >= 2 * CAP).astype(jnp.int32) + (j >= 3 * CAP).astype(jnp.int32)
    slotj = (j - dCj * CAP).astype(jnp.float32)

    def pack(p, db):
        A, B, C = ORDERS[p]
        gw = GB[p] * 128
        bb = wrap(co[B] + db)

        def one(a, carry):
            codes = jnp.concatenate([jnp.broadcast_to(rc[p, bb * 4 + a, wrap(co[C] + dc)], (CAP, 128)) for dc in range(4)], axis=0)
            sel = jnp.where(codes == slotj, 1.0, 0.0).astype(jnp.bfloat16)
            rows = jnp.dot(sel, gb[p][bb, a, :, 0:gw], preferred_element_type=jnp.float32)
            rows = rows.reshape(4, CAP, gw).astype(jnp.bfloat16)
            for dc in range(4):
                if db == 2 and dc == 0:
                    if A < C:
                        lv[p][a, co[C]] = rows[0]
                    else:
                        lv[p][co[C], a] = rows[0]
                else:
                    sc[p][dc, db % 4, a] = rows[dc]
            return carry
        lax.fori_loop(0, 4, one, 0)
        for dc in (1, 3, 2):
            go(rcopy(sc[p].at[dc, db % 4], fdst(p, db, 0), gcs.at[p, db % 4, dc - 1], gcr.at[p, db % 4, dc - 1], C, dc))
        if db != 2:
            cp = pltpu.make_async_copy(sc[p].at[0, db % 4], fdst(p, db, 0), gcl.at[p, db % 4])
            cp.start()
            locals_[p, db % 4] = cp

    def fdst(p, db, d):
        A, B, C = ORDERS[p]
        if db == 2:
            c = wrap(co[C] - d)
            return lv[p].at[:, c] if A < C else lv[p].at[c, :]
        idx = [None, None, None]
        idx[A] = slice(None)
        idx[B] = wrap(co[B] + db)
        idx[C] = wrap(co[C] - d)
        return F.at[idx[0], idx[1], idx[2], :, pl.ds(gcol[p], GB[p] * 128)]

    def hdst(p, bb, d):
        A, B, C = ORDERS[p]
        idx = [None, None, None]
        idx[A] = slice(None)
        idx[B] = bb
        idx[C] = wrap(co[C] - d)
        return HV.at[idx[0], idx[1], idx[2], :, pl.ds(hcol[p], HB[p] * 128)]

    locals_ = {}
    hbcp = {}
    for p, (A, B, C) in enumerate(ORDERS):
        for d in (1, 3, 2):
            hacp[p, d].wait_recv()
        for d in (1, 3, 2):
            hbcp[p, d] = go(rcopy(hb[p].at[wrap(co[B] + d)], hc[p].at[d - 1], hbs.at[p, d - 1], hbr.at[p, d - 1], B, d))
    for p in range(3):
        pltpu.make_async_copy(rc.at[p, pl.ds(0, 15)], rc.at[p, pl.ds(0, 15)], trs.at[p]).wait()
        pack(p, 0)
    for k in range(4):
        for p in range(3):
            bcp[p, k][0].wait_recv(); go(bcp[p, k][2])
            bcp[p, k][1].wait_recv(); go(bcp[p, k][3])

    def hidden_c(p, d):
        A, B, C = ORDERS[p]
        bb = wrap(co[B] - d)
        for dc in (1, 3, 2, 0):
            cs = wrap(co[C] + dc)
            src = hb[p].at[co[B], :, cs] if d == 0 else hc[p].at[d - 1, :, cs]
            if dc == 0:
                dst = hdst(p, bb, 0)
                for a in range(4):
                    dst[a] = src[a]
            else:
                go(rcopy(src, hdst(p, bb, 0), hcs.at[p, d, dc - 1], hcr.at[p, d, dc - 1], C, dc))
    for p in range(3):
        hidden_c(p, 0)
    for p in range(3):
        pack(p, -1)
    for p in range(3):
        pack(p, 1)
    for p in range(3):
        for d in (1, 3, 2):
            hbcp[p, d].wait_recv()
            hidden_c(p, d)
    for p in range(3):
        for k in range(4):
            bcp[p, k][2].wait_recv(); bcp[p, k][3].wait_recv()
        pack(p, 2)
    for p, (A, B, C) in enumerate(ORDERS):
        for d in range(4):
            for dc in (1, 3, 2):
                src = hc[p].at[max(d - 1, 0), :, 0]
                rcopy(src, hdst(p, wrap(co[B] - d), dc), hcs.at[p, d, dc - 1], hcr.at[p, d, dc - 1], C, dc).wait_recv()
    hout = pltpu.make_async_copy(HV, HR, hos.at[0])
    hout.start()
    wload.wait()

    def rest(p):
        return tuple(ax for ax in range(3) if ax != ORDERS[p][1])

    def at_b(ref, p, bb):
        idx = [slice(None)] * 3
        idx[ORDERS[p][1]] = bb
        return ref.at[idx[0], idx[1], idx[2]]

    chunks = [(p, db) for db in (0, -1, 1) for p in range(3)]

    def arrived(p, db):
        for dc in (1, 3, 2):
            rcopy(sc[p].at[dc, db % 4], fdst(p, db, dc), gcs.at[p, db % 4, dc - 1], gcr.at[p, db % 4, dc - 1], ORDERS[p][2], dc).wait_recv()
        if db != 2:
            locals_[p, db % 4].wait()

    for p in range(3):
        view = at_b(HV, p, wrap(co[ORDERS[p][1]] + 2))
        for i in range(4):
            g2[i * 96:(i + 1) * 96, 0:1024] = view[i].astype(f32).reshape(96, 1024).astype(bf)

        def prod(ct, carry, p=p):
            cols = pl.ds(pl.multiple_of(ct * 256, 256), 256)
            wcols = pl.ds(pl.multiple_of(gcol[p] + ct * 256, 256), 256)
            u = jnp.dot(g2[:, 0:1024], wv[:, wcols], preferred_element_type=f32)
            U[p][:, :, :, cols] = u.reshape(4, 4, CAP, 256).astype(bf)
            return carry
        lax.fori_loop(0, GB[p] // 2, prod, 0)

    def load(n):
        p, db = chunks[n]
        bb = wrap(co[ORDERS[p][1]] + db)
        arrived(p, db)
        gw = GB[p] * 128
        cp = pltpu.make_async_copy(at_b(F, p, bb).at[:, :, :, pl.ds(gcol[p], gw)], gch.at[n % 2, :, :, :, pl.ds(0, gw)], gls.at[n % 2])
        cp.start()
        return cp

    def derive(n):
        p, db = chunks[n]
        gw = GB[p] * 128
        B = ORDERS[p][1]
        bb = wrap(co[B] + db)
        R1, R2 = rest(p)
        for i in range(4):
            g2[i * 96:(i + 1) * 96, 0:gw] = gch[n % 2, i, :, :, 0:gw].astype(f32).reshape(96, gw).astype(bf)
        hview = at_b(HV, p, bb)
        acc = jnp.zeros((384, 128), f32)
        for f in range(4):
            proj = lax.dot_general(g2[:, 0:gw], wv[f * 256:(f + 1) * 256, gcol[p]:gcol[p] + gw], (((1,), (1,)), ((), ())),
                                   preferred_element_type=f32)
            q = proj * hview[:, :, :, f * 256:(f + 1) * 256].astype(f32).reshape(384, 256)
            acc = acc + q[:, 0:128] + q[:, 128:256]
        give(p, db, acc)

    def give(p, db, acc):
        B = ORDERS[p][1]
        bb = wrap(co[B] + db)
        R1, R2 = rest(p)
        pad = jnp.concatenate([acc.reshape(16, CAP, 128), jnp.zeros((16, 8, 128), f32)], axis=1).reshape(512, 128)
        row = jnp.sum(jnp.transpose(pad), axis=0, keepdims=True)
        for i in range(4):
            ds[p, db % 4, i] = row[:, i * 128:(i + 1) * 128]
        for d1 in range(4):
            for d2 in range(4):
                i = wrap(co[R1] + d1)
                if (db, d1, d2) == (0, 0, 0):
                    dr[p, e] = ds[p, 0, i]
                    continue
                c = [None] * 3
                c[R1], c[R2], c[B] = i, wrap(co[R2] + d2), bb
                pltpu.make_async_remote_copy(src_ref=ds.at[p, db % 4, i], dst_ref=dr.at[p, e], send_sem=dss.at[p], recv_sem=drs.at[p],
                                             device_id={"expert": c[0] * 16 + c[1] * 4 + c[2]}, device_id_type=MESH).start()

    cur = load(0)
    for n in range(9):
        nxt = load(n + 1) if n < 8 else None
        cur.wait()
        derive(n)
        cur = nxt
    lcps = []
    for p in range(3):
        arrived(p, 2)
        cp = pltpu.make_async_copy(lv[p], at_b(F, p, wrap(co[ORDERS[p][1]] + 2)).at[:, :, :, pl.ds(gcol[p], GB[p] * 128)], lvs.at[p])
        cp.start()
        lcps.append(cp)
        quads = []
        for i in range(4):
            t = jnp.zeros((4, CAP, 128), f32)
            for k in range(GB[p]):
                cols = slice(k * 128, (k + 1) * 128)
                t = t + U[p][i, :, :, cols].astype(f32) * lv[p][i, :, :, cols].astype(f32)
            quads.append(t.reshape(96, 128))
        give(p, 2, jnp.concatenate(quads, axis=0))

    home = jnp.zeros((64, 128), f32)
    window = lax.broadcasted_iota(jnp.int32, (64, 128), 1) // 32
    for p in range(3):
        pltpu.make_async_copy(dr.at[p, pl.ds(0, 63)], dr.at[p, pl.ds(0, 63)], drs.at[p]).wait()
        home = home + jnp.where(window == co[rest(p)[1]], dr[p].reshape(64, 128), 0.0)
    home = home + pltpu.roll(home, 64, 1)
    home = home + pltpu.roll(home, 32, 1)
    code_e = codes_s[...]
    score_e = score_s[...]
    rd = jnp.zeros((64, 128), f32)
    for s in range(CAP):
        rd = rd + jnp.where(code_e == float(s), home[:, s:s + 1], 0.0)
    tot = jnp.sum(score_e, axis=0, keepdims=True)
    weight = score_e / tot
    on = code_e >= 0.0
    rd = jnp.where(on, rd / jnp.where(on, weight.astype(bf).astype(f32), 1.0), 0.0)
    center = jnp.sum(weight * rd, axis=0, keepdims=True)
    logit = score_e * (1.0 - score_e) / tot * (rd - center)
    lt = jnp.transpose(logit).astype(bf)
    hcps = []
    for p, (A, B, C) in enumerate(ORDERS):
        gw = GB[p] * 128
        for c0 in range(0, gw, 256):
            add = jnp.dot(lt, router[:, gcol[p] + c0:gcol[p] + c0 + 256], preferred_element_type=f32)
            hnd[:, gcol[p] + c0:gcol[p] + c0 + 256] = (gb[p][co[B], co[A], :, c0:c0 + 256].astype(f32) + add).astype(bf)
        cols = pl.ds(gcol[p], gw)
        cp = pltpu.make_async_copy(hnd.at[:, cols], handed.at[:, cols], gls.at[p])
        cp.start()
        hcps.append(cp)
    for p in range(3):
        pltpu.make_async_copy(dr.at[p, pl.ds(0, 63)], dr.at[p, pl.ds(0, 63)], dss.at[p]).wait()
    for p in range(3):
        pltpu.make_async_copy(rc.at[p, pl.ds(0, 15)], rc.at[p, pl.ds(0, 15)], tss.at[p]).wait()
    for cp in lcps:
        cp.wait()
    hout.wait()
    for cp in sends:
        cp.wait_send()
    for cp in hcps:
        cp.wait()


def exchange(routes, scores, router, grad, hidden, down):
    bf, f32 = jnp.bfloat16, jnp.float32
    V = pltpu.VMEM
    D = pltpu.SemaphoreType.DMA
    any_ = pl.BlockSpec(memory_space=pl.ANY)
    vm = pl.BlockSpec(memory_space=pltpu.VMEM)
    gmax = max(GB) * 128
    F, HR, handed = pl.pallas_call(
        comm_kernel,
        out_shape=(jax.ShapeDtypeStruct((4, 4, 4, CAP, 4096), bf), jax.ShapeDtypeStruct((4, 4, 4, CAP, 1024), bf),
                   jax.ShapeDtypeStruct((128, 4096), bf)),
        in_specs=[vm, vm, vm, any_, any_, any_], out_specs=(any_, any_, any_),
        scratch_shapes=[V((1024, 1024), bf), V((4, 4, 4, CAP, 1024), bf), V((1024, 4096), bf), V((2, 4, 4, CAP, gmax), bf),
                        V((384, gmax), bf), V((3, 4, 4, 1, 128), f32), V((3, 64, 1, 128), f32), V((128, 4096), bf),
                        V((64, 128), f32), V((64, 128), f32), V((4, 4, 4, 1, 128), f32), V((3, 16, 4, 1, 128), f32)]
        + [V((4, 4, CAP, g * 128), bf) for g in GB] * 2
        + [V((4, 4, 128, g * 128), bf) for g in GB]
        + [V((4, 4, 4, CAP, g * 128), bf) for g in GB]
        + [V((3, 4, 4, CAP, h * 128), bf) for h in HB]
        + [V((4, 4, 4, CAP, h * 128), bf) for h in HB]
        + [V((3, 4, 4, CAP, h * 128), bf) for h in HB]
        + [D((3, 2)), D((3, 4)), D((3, 4)), D((3, 4, 4)), D((3, 4, 4)), D((3, 4, 3)), D((3, 4, 3)), D((3, 4)),
           D((3, 3)), D((3, 3)), D((3, 3)), D((3, 3)), D((3, 4, 3)), D((3, 4, 3)),
           D((3,)), D((1,)), D((3,)), D((3,)), D((1,)), D((3,)), D((3,)), D((3,))],
        compiler_params=pltpu.CompilerParams(has_side_effects=True, collective_id=0, vmem_limit_bytes=67043328),
    )(routes, scores, router, grad, hidden, down)
    return F.reshape(64 * CAP, 4096), HR.reshape(64 * CAP, 1024), handed


def body(grad_out, saved_hidden, routes, scores, down_weight, router):
    n_tokens, n_routes, hidden_width = saved_hidden.shape[1:]
    hidden_flat = saved_hidden[0].reshape(n_tokens * n_routes, hidden_width)
    grad_recv, hidden_recv, inp = exchange(routes[0].T, scores[0].T, router[0], grad_out[0], hidden_flat, down_weight[0, 0])
    handed = lax.ppermute(inp, "section", [(0, 1), (1, 0)])
    weight_out = lax.dot_general(hidden_recv, grad_recv, (((0,), (0,)), ((), ())), preferred_element_type=jnp.float32).astype(jnp.bfloat16)
    return weight_out[None, None], handed[None]


def solution(mesh):
    return jax.shard_map(
        body, mesh=mesh,
        in_specs=(P("section", "expert", None), P("section", "expert", None, None), P("section", "expert", None),
                  P("section", "expert", None), P("section", "expert", None, None), P("section", None, None)),
        out_specs=(P("section", "expert", None, None), P("section", "expert", None)), check_vma=False)
```

```python
import functools
import jax
import jax.numpy as jnp
from jax import lax
from jax.experimental import pallas as pl
from jax.experimental.pallas import tpu as pltpu
from jax.sharding import PartitionSpec as P

MESH = pl.DeviceIdType.MESH
CAP = 24
ORDERS = ((0, 1, 2), (1, 2, 0), (2, 0, 1))
STRIDE = (16, 4, 1)
GB = (10, 12, 10)
HB = (2, 3, 3)


def starts(blocks):
    return tuple(128 * sum(blocks[:i]) for i in range(len(blocks)))


def comm_kernel(routes, scores, router, grad, hidden, down, F, HR, handed, hid, HV, wv, gch, g2, ds, dr, hnd, codes_s, score_s, tab, rc, U0, U1, U2, lv0, lv1, lv2,
                gb0, gb1, gb2, sc0, sc1, sc2, ha0, ha1, ha2, hb0, hb1, hb2, hc0, hc1, hc2,
                lsem, gas, gar, gbs, gbr, gcs, gcr, gcl, has, har, hbs, hbr, hcs, hcr, gls, wsem, dss, drs, hos, lvs, tss, trs):
    gb, sc, ha, hb, hc = (gb0, gb1, gb2), (sc0, sc1, sc2), (ha0, ha1, ha2), (hb0, hb1, hb2), (hc0, hc1, hc2)
    e = lax.axis_index("expert")
    co = (e // 16, (e // 4) % 4, e % 4)
    gcol, hcol = starts(GB), starts(HB)
    U, lv = (U0, U1, U2), (lv0, lv1, lv2)

    def wrap(v):
        return lax.rem(v + 4, 4)

    def peer(axis, delta):
        c = list(co)
        c[axis] = wrap(co[axis] + delta)
        return {"expert": c[0] * 16 + c[1] * 4 + c[2]}

    def rcopy(src, dst, ss, rs, axis, delta):
        return pltpu.make_async_remote_copy(src_ref=src, dst_ref=dst, send_sem=ss, recv_sem=rs,
                                            device_id=peer(axis, delta), device_id_type=MESH)

    def plane(p, da, db):
        A, B, C = ORDERS[p]
        c = list(co)
        c[A], c[B] = wrap(co[A] + da), wrap(co[B] + db)
        return c, {"expert": c[0] * 16 + c[1] * 4 + c[2]}

    barrier = pltpu.get_barrier_semaphore()
    for axis in range(3):
        for d in (1, 2, 3):
            pl.semaphore_signal(barrier, inc=1, device_id=peer(axis, d), device_id_type=MESH)
    for p in range(3):
        for da in (1, 2, 3):
            for db in (1, 2, 3):
                pl.semaphore_signal(barrier, inc=1, device_id=plane(p, da, db)[1], device_id_type=MESH)

    sends = []

    def go(cp):
        cp.start()
        sends.append(cp)
        return cp

    loads = []
    for p, (A, B, C) in enumerate(ORDERS):
        gw = GB[p] * 128
        own = gb[p].at[co[B], co[A]]
        l0 = pltpu.make_async_copy(grad.at[:, pl.ds(gcol[p], gw)], own.at[:, pl.ds(0, gw)], lsem.at[p, 0])
        l0.start()
        loads.append(l0)
    hload = pltpu.make_async_copy(hidden, hid, lsem.at[0, 1])
    hload.start()
    wload = pltpu.make_async_copy(down, wv, wsem.at[0])
    wload.start()

    def ring(p, axis, slot_of, sems, semr, idx):
        gw = GB[p] * 128
        half = (gw // 256) * 128
        def cp(i, src_delta, cols, delta):
            ref = slot_of(src_delta)
            if cols is not None:
                ref = ref.at[:, pl.ds(*cols)]
            return rcopy(ref, ref, sems.at[idx + (i,)], semr.at[idx + (i,)], axis, delta)
        return (cp(0, 0, None, 1), cp(1, 0, None, -1), cp(2, -1, (0, half), 1), cp(3, 1, (half, gw - half), -1))

    acp, bcp = [], {}
    for p, (A, B, C) in enumerate(ORDERS):
        acp.append(ring(p, A, lambda d, p=p, A=A, B=B: gb[p].at[co[B], wrap(co[A] + d)], gas, gar, (p,)))
        for k, da in enumerate((0, -1, 1, 2)):
            bcp[p, k] = ring(p, B, lambda d, p=p, A=A, B=B, da=da: gb[p].at[wrap(co[B] + d), wrap(co[A] + da)], gbs, gbr, (p, k))
    pl.semaphore_wait(barrier, 36)
    for p in range(3):
        loads[p].wait()
        go(acp[p][0]); go(acp[p][1])
    for p in range(3):
        go(bcp[p, 0][0]); go(bcp[p, 0][1])

    f32, bf = jnp.float32, jnp.bfloat16
    ri = routes[...].astype(f32)
    st = scores[...]
    tot = jnp.sum(st, axis=0, keepdims=True)
    low = (st / tot).astype(bf)
    eio = lax.broadcasted_iota(jnp.int32, (64, 128), 0).astype(f32)
    member = jnp.zeros((64, 128), f32)
    score_e = jnp.zeros((64, 128), f32)
    for k in range(8):
        hit = eio == ri[k:k + 1, :]
        member = member + jnp.where(hit, 1.0, 0.0)
        score_e = score_e + jnp.where(hit, st[k:k + 1, :], 0.0)
    before = lax.broadcasted_iota(jnp.int32, (128, 128), 0) < lax.broadcasted_iota(jnp.int32, (128, 128), 1)
    rank = jnp.dot(member.astype(bf), jnp.where(before, 1.0, 0.0).astype(bf), preferred_element_type=f32)
    code_e = jnp.where(member > 0.0, rank, -1.0)
    codes_s[...] = code_e
    score_s[...] = score_e
    for k in range(64):
        tab[k // 16, (k // 4) % 4, k % 4] = code_e[k:k + 1, :]

    for p, (A, B, C) in enumerate(ORDERS):
        for da in range(4):
            for db in range(4):
                c, dev = plane(p, da, db)
                idx = list(c)
                if da == 0 and db == 0:
                    for k in range(4):
                        idx[C] = k
                        rc[p, co[B] * 4 + co[A], k] = tab[idx[0], idx[1], idx[2]]
                    continue
                idx[C] = slice(None)
                pltpu.make_async_remote_copy(src_ref=tab.at[idx[0], idx[1], idx[2]], dst_ref=rc.at[p, co[B] * 4 + co[A]],
                                             send_sem=tss.at[p], recv_sem=trs.at[p], device_id=dev, device_id_type=MESH).start()

    slots = jnp.concatenate([jnp.sum(jnp.where(eio == ri[k:k + 1, :], rank, 0.0), axis=0, keepdims=True) for k in range(8)], axis=0)
    n8 = lax.broadcasted_iota(jnp.int32, (128, 1024), 1) // 8
    spread = jnp.where(n8 == lax.broadcasted_iota(jnp.int32, (128, 1024), 0), 1.0, 0.0).astype(bf)
    mine = lax.broadcasted_iota(jnp.int32, (8, 1024), 1) % 8 == lax.broadcasted_iota(jnp.int32, (8, 1024), 0)

    def lanes(v):
        return jnp.sum(jnp.where(mine, jnp.dot(v.astype(bf), spread, preferred_element_type=f32), 0.0), axis=0, keepdims=True)
    tgt = CAP * lanes(ri) + lanes(slots)
    wgt = lanes(low)
    hload.wait()

    for p, (A, B, C) in enumerate(ORDERS):
        hw = HB[p] * 128
        r = lax.broadcasted_iota(jnp.int32, (16 * CAP, 1), 0)
        dB = (r >= 4 * CAP).astype(jnp.int32) + (r >= 8 * CAP).astype(jnp.int32) + (r >= 12 * CAP).astype(jnp.int32)
        r1 = r - dB * (4 * CAP)
        dC = (r1 >= CAP).astype(jnp.int32) + (r1 >= 2 * CAP).astype(jnp.int32) + (r1 >= 3 * CAP).astype(jnp.int32)
        slot = r1 - dC * CAP
        base = CAP * (dB * STRIDE[B] + dC * STRIDE[C]) + slot
        for d in (1, 3, 2, 0):
            code = base + CAP * STRIDE[A] * wrap(co[A] + d)
            pick = jnp.where(code.astype(f32) == tgt, wgt, 0.0).astype(jnp.bfloat16)
            rows = jnp.dot(pick, hid[:, hcol[p]:hcol[p] + hw], preferred_element_type=jnp.float32)
            rows = rows.reshape(4, 4, CAP, hw).astype(jnp.bfloat16)
            if d == 0:
                for j in range(4):
                    hb[p][j, co[A]] = rows[j]
            else:
                ha[p][d - 1] = rows
                go(rcopy(ha[p].at[d - 1], hb[p].at[:, co[A]], has.at[p, d - 1], har.at[p, d - 1], A, d))
    hacp = {}
    for p, (A, B, C) in enumerate(ORDERS):
        for d in (1, 2, 3):
            hacp[p, d] = rcopy(ha[p].at[d - 1], hb[p].at[:, wrap(co[A] - d)], has.at[p, d - 1], har.at[p, d - 1], A, d)

    for p in range(3):
        acp[p][0].wait_recv(); go(acp[p][2])
        acp[p][1].wait_recv(); go(acp[p][3])
    for p in range(3):
        for k in (1, 2):
            go(bcp[p, k][0]); go(bcp[p, k][1])
    for p in range(3):
        acp[p][2].wait_recv(); acp[p][3].wait_recv()
        go(bcp[p, 3][0]); go(bcp[p, 3][1])

    j = lax.broadcasted_iota(jnp.int32, (4 * CAP, 1), 0)
    dCj = (j >= CAP).astype(jnp.int32) + (j >= 2 * CAP).astype(jnp.int32) + (j >= 3 * CAP).astype(jnp.int32)
    slotj = (j - dCj * CAP).astype(jnp.float32)

    def pack(p, db):
        A, B, C = ORDERS[p]
        gw = GB[p] * 128
        bb = wrap(co[B] + db)

        def one(a, carry):
            codes = jnp.concatenate([jnp.broadcast_to(rc[p, bb * 4 + a, wrap(co[C] + dc)], (CAP, 128)) for dc in range(4)], axis=0)
            sel = jnp.where(codes == slotj, 1.0, 0.0).astype(jnp.bfloat16)
            rows = jnp.dot(sel, gb[p][bb, a, :, 0:gw], preferred_element_type=jnp.float32)
            rows = rows.reshape(4, CAP, gw).astype(jnp.bfloat16)
            for dc in range(4):
                if db == 2 and dc == 0:
                    if A < C:
                        lv[p][a, co[C]] = rows[0]
                    else:
                        lv[p][co[C], a] = rows[0]
                else:
                    sc[p][dc, db % 4, a] = rows[dc]
            return carry
        lax.fori_loop(0, 4, one, 0)
        for dc in (1, 3, 2):
            go(rcopy(sc[p].at[dc, db % 4], fdst(p, db, 0), gcs.at[p, db % 4, dc - 1], gcr.at[p, db % 4, dc - 1], C, dc))
        if db != 2:
            cp = pltpu.make_async_copy(sc[p].at[0, db % 4], fdst(p, db, 0), gcl.at[p, db % 4])
            cp.start()
            locals_[p, db % 4] = cp

    def fdst(p, db, d):
        A, B, C = ORDERS[p]
        if db == 2:
            c = wrap(co[C] - d)
            return lv[p].at[:, c] if A < C else lv[p].at[c, :]
        idx = [None, None, None]
        idx[A] = slice(None)
        idx[B] = wrap(co[B] + db)
        idx[C] = wrap(co[C] - d)
        return F.at[idx[0], idx[1], idx[2], :, pl.ds(gcol[p], GB[p] * 128)]

    def hdst(p, bb, d):
        A, B, C = ORDERS[p]
        idx = [None, None, None]
        idx[A] = slice(None)
        idx[B] = bb
        idx[C] = wrap(co[C] - d)
        return HV.at[idx[0], idx[1], idx[2], :, pl.ds(hcol[p], HB[p] * 128)]

    locals_ = {}
    hbcp = {}
    for p, (A, B, C) in enumerate(ORDERS):
        for d in (1, 3, 2):
            hacp[p, d].wait_recv()
        for d in (1, 3, 2):
            hbcp[p, d] = go(rcopy(hb[p].at[wrap(co[B] + d)], hc[p].at[d - 1], hbs.at[p, d - 1], hbr.at[p, d - 1], B, d))
    for p in range(3):
        pltpu.make_async_copy(rc.at[p, pl.ds(0, 15)], rc.at[p, pl.ds(0, 15)], trs.at[p]).wait()
        pack(p, 0)
    for k in range(4):
        for p in range(3):
            bcp[p, k][0].wait_recv(); go(bcp[p, k][2])
            bcp[p, k][1].wait_recv(); go(bcp[p, k][3])

    def hidden_c(p, d):
        A, B, C = ORDERS[p]
        bb = wrap(co[B] - d)
        for dc in (1, 3, 2, 0):
            cs = wrap(co[C] + dc)
            src = hb[p].at[co[B], :, cs] if d == 0 else hc[p].at[d - 1, :, cs]
            if dc == 0:
                dst = hdst(p, bb, 0)
                for a in range(4):
                    dst[a] = src[a]
            else:
                go(rcopy(src, hdst(p, bb, 0), hcs.at[p, d, dc - 1], hcr.at[p, d, dc - 1], C, dc))
    for p in range(3):
        hidden_c(p, 0)
    for p in range(3):
        for d in (1, 3, 2):
            hbcp[p, d].wait_recv()
            hidden_c(p, d)
    for p in range(3):
        pack(p, -1)
    for p in range(3):
        pack(p, 1)
    for p in range(3):
        for k in range(4):
            bcp[p, k][2].wait_recv(); bcp[p, k][3].wait_recv()
        pack(p, 2)
    for p, (A, B, C) in enumerate(ORDERS):
        for d in range(4):
            for dc in (1, 3, 2):
                src = hc[p].at[max(d - 1, 0), :, 0]
                rcopy(src, hdst(p, wrap(co[B] - d), dc), hcs.at[p, d, dc - 1], hcr.at[p, d, dc - 1], C, dc).wait_recv()
    hout = pltpu.make_async_copy(HV, HR, hos.at[0])
    hout.start()
    wload.wait()

    def rest(p):
        return tuple(ax for ax in range(3) if ax != ORDERS[p][1])

    def at_b(ref, p, bb):
        idx = [slice(None)] * 3
        idx[ORDERS[p][1]] = bb
        return ref.at[idx[0], idx[1], idx[2]]

    chunks = [(p, db) for db in (0, -1, 1) for p in range(3)]

    def arrived(p, db):
        for dc in (1, 3, 2):
            rcopy(sc[p].at[dc, db % 4], fdst(p, db, dc), gcs.at[p, db % 4, dc - 1], gcr.at[p, db % 4, dc - 1], ORDERS[p][2], dc).wait_recv()
        if db != 2:
            locals_[p, db % 4].wait()

    for p in range(3):
        view = at_b(HV, p, wrap(co[ORDERS[p][1]] + 2))
        for i in range(4):
            g2[i * 96:(i + 1) * 96, 0:1024] = view[i].astype(f32).reshape(96, 1024).astype(bf)

        def prod(ct, carry, p=p):
            cols = pl.ds(pl.multiple_of(ct * 256, 256), 256)
            wcols = pl.ds(pl.multiple_of(gcol[p] + ct * 256, 256), 256)
            u = jnp.dot(g2[:, 0:1024], wv[:, wcols], preferred_element_type=f32)
            U[p][:, :, :, cols] = u.reshape(4, 4, CAP, 256).astype(bf)
            return carry
        lax.fori_loop(0, GB[p] // 2, prod, 0)

    def load(n):
        p, db = chunks[n]
        bb = wrap(co[ORDERS[p][1]] + db)
        arrived(p, db)
        gw = GB[p] * 128
        cp = pltpu.make_async_copy(at_b(F, p, bb).at[:, :, :, pl.ds(gcol[p], gw)], gch.at[n % 2, :, :, :, pl.ds(0, gw)], gls.at[n % 2])
        cp.start()
        return cp

    def derive(n):
        p, db = chunks[n]
        gw = GB[p] * 128
        B = ORDERS[p][1]
        bb = wrap(co[B] + db)
        R1, R2 = rest(p)
        for i in range(4):
            g2[i * 96:(i + 1) * 96, 0:gw] = gch[n % 2, i, :, :, 0:gw].astype(f32).reshape(96, gw).astype(bf)
        hview = at_b(HV, p, bb)
        acc = jnp.zeros((384, 128), f32)
        for f in range(4):
            proj = lax.dot_general(g2[:, 0:gw], wv[f * 256:(f + 1) * 256, gcol[p]:gcol[p] + gw], (((1,), (1,)), ((), ())),
                                   preferred_element_type=f32)
            q = proj * hview[:, :, :, f * 256:(f + 1) * 256].astype(f32).reshape(384, 256)
            acc = acc + q[:, 0:128] + q[:, 128:256]
        give(p, db, acc)

    def give(p, db, acc):
        B = ORDERS[p][1]
        bb = wrap(co[B] + db)
        R1, R2 = rest(p)
        pad = jnp.concatenate([acc.reshape(16, CAP, 128), jnp.zeros((16, 8, 128), f32)], axis=1).reshape(512, 128)
        row = jnp.sum(jnp.transpose(pad), axis=0, keepdims=True)
        for i in range(4):
            ds[p, db % 4, i] = row[:, i * 128:(i + 1) * 128]
        for d1 in range(4):
            for d2 in range(4):
                i = wrap(co[R1] + d1)
                if (db, d1, d2) == (0, 0, 0):
                    dr[p, e] = ds[p, 0, i]
                    continue
                c = [None] * 3
                c[R1], c[R2], c[B] = i, wrap(co[R2] + d2), bb
                pltpu.make_async_remote_copy(src_ref=ds.at[p, db % 4, i], dst_ref=dr.at[p, e], send_sem=dss.at[p], recv_sem=drs.at[p],
                                             device_id={"expert": c[0] * 16 + c[1] * 4 + c[2]}, device_id_type=MESH).start()

    cur = load(0)
    for n in range(9):
        nxt = load(n + 1) if n < 8 else None
        cur.wait()
        derive(n)
        cur = nxt
    lcps = []
    for p in range(3):
        arrived(p, 2)
        cp = pltpu.make_async_copy(lv[p], at_b(F, p, wrap(co[ORDERS[p][1]] + 2)).at[:, :, :, pl.ds(gcol[p], GB[p] * 128)], lvs.at[p])
        cp.start()
        lcps.append(cp)
        quads = []
        for i in range(4):
            t = jnp.zeros((4, CAP, 128), f32)
            for k in range(GB[p]):
                cols = slice(k * 128, (k + 1) * 128)
                t = t + U[p][i, :, :, cols].astype(f32) * lv[p][i, :, :, cols].astype(f32)
            quads.append(t.reshape(96, 128))
        give(p, 2, jnp.concatenate(quads, axis=0))

    home = jnp.zeros((64, 128), f32)
    window = lax.broadcasted_iota(jnp.int32, (64, 128), 1) // 32
    for p in range(3):
        pltpu.make_async_copy(dr.at[p, pl.ds(0, 63)], dr.at[p, pl.ds(0, 63)], drs.at[p]).wait()
        home = home + jnp.where(window == co[rest(p)[1]], dr[p].reshape(64, 128), 0.0)
    home = home + pltpu.roll(home, 64, 1)
    home = home + pltpu.roll(home, 32, 1)
    code_e = codes_s[...]
    score_e = score_s[...]
    rd = jnp.zeros((64, 128), f32)
    for s in range(CAP):
        rd = rd + jnp.where(code_e == float(s), home[:, s:s + 1], 0.0)
    tot = jnp.sum(score_e, axis=0, keepdims=True)
    weight = score_e / tot
    on = code_e >= 0.0
    rd = jnp.where(on, rd / jnp.where(on, weight.astype(bf).astype(f32), 1.0), 0.0)
    center = jnp.sum(weight * rd, axis=0, keepdims=True)
    logit = score_e * (1.0 - score_e) / tot * (rd - center)
    lt = jnp.transpose(logit).astype(bf)
    hcps = []
    for p, (A, B, C) in enumerate(ORDERS):
        gw = GB[p] * 128
        for c0 in range(0, gw, 256):
            add = jnp.dot(lt, router[:, gcol[p] + c0:gcol[p] + c0 + 256], preferred_element_type=f32)
            hnd[:, gcol[p] + c0:gcol[p] + c0 + 256] = (gb[p][co[B], co[A], :, c0:c0 + 256].astype(f32) + add).astype(bf)
        cols = pl.ds(gcol[p], gw)
        cp = pltpu.make_async_copy(hnd.at[:, cols], handed.at[:, cols], gls.at[p])
        cp.start()
        hcps.append(cp)
    for p in range(3):
        pltpu.make_async_copy(dr.at[p, pl.ds(0, 63)], dr.at[p, pl.ds(0, 63)], dss.at[p]).wait()
    for p in range(3):
        pltpu.make_async_copy(rc.at[p, pl.ds(0, 15)], rc.at[p, pl.ds(0, 15)], tss.at[p]).wait()
    for cp in lcps:
        cp.wait()
    hout.wait()
    for cp in sends:
        cp.wait_send()
    for cp in hcps:
        cp.wait()


def exchange(routes, scores, router, grad, hidden, down):
    bf, f32 = jnp.bfloat16, jnp.float32
    V = pltpu.VMEM
    D = pltpu.SemaphoreType.DMA
    any_ = pl.BlockSpec(memory_space=pl.ANY)
    vm = pl.BlockSpec(memory_space=pltpu.VMEM)
    gmax = max(GB) * 128
    F, HR, handed = pl.pallas_call(
        comm_kernel,
        out_shape=(jax.ShapeDtypeStruct((4, 4, 4, CAP, 4096), bf), jax.ShapeDtypeStruct((4, 4, 4, CAP, 1024), bf),
                   jax.ShapeDtypeStruct((128, 4096), bf)),
        in_specs=[vm, vm, vm, any_, any_, any_], out_specs=(any_, any_, any_),
        scratch_shapes=[V((1024, 1024), bf), V((4, 4, 4, CAP, 1024), bf), V((1024, 4096), bf), V((2, 4, 4, CAP, gmax), bf),
                        V((384, gmax), bf), V((3, 4, 4, 1, 128), f32), V((3, 64, 1, 128), f32), V((128, 4096), bf),
                        V((64, 128), f32), V((64, 128), f32), V((4, 4, 4, 1, 128), f32), V((3, 16, 4, 1, 128), f32)]
        + [V((4, 4, CAP, g * 128), bf) for g in GB] * 2
        + [V((4, 4, 128, g * 128), bf) for g in GB]
        + [V((4, 4, 4, CAP, g * 128), bf) for g in GB]
        + [V((3, 4, 4, CAP, h * 128), bf) for h in HB]
        + [V((4, 4, 4, CAP, h * 128), bf) for h in HB]
        + [V((3, 4, 4, CAP, h * 128), bf) for h in HB]
        + [D((3, 2)), D((3, 4)), D((3, 4)), D((3, 4, 4)), D((3, 4, 4)), D((3, 4, 3)), D((3, 4, 3)), D((3, 4)),
           D((3, 3)), D((3, 3)), D((3, 3)), D((3, 3)), D((3, 4, 3)), D((3, 4, 3)),
           D((3,)), D((1,)), D((3,)), D((3,)), D((1,)), D((3,)), D((3,)), D((3,))],
        compiler_params=pltpu.CompilerParams(has_side_effects=True, collective_id=0, vmem_limit_bytes=67043328),
    )(routes, scores, router, grad, hidden, down)
    return F.reshape(64 * CAP, 4096), HR.reshape(64 * CAP, 1024), handed


def body(grad_out, saved_hidden, routes, scores, down_weight, router):
    n_tokens, n_routes, hidden_width = saved_hidden.shape[1:]
    hidden_flat = saved_hidden[0].reshape(n_tokens * n_routes, hidden_width)
    grad_recv, hidden_recv, inp = exchange(routes[0].T, scores[0].T, router[0], grad_out[0], hidden_flat, down_weight[0, 0])
    handed = lax.ppermute(inp, "section", [(0, 1), (1, 0)])
    weight_out = lax.dot_general(hidden_recv, grad_recv, (((0,), (0,)), ((), ())), preferred_element_type=jnp.float32).astype(jnp.bfloat16)
    return weight_out[None, None], handed[None]


def solution(mesh):
    return jax.shard_map(
        body, mesh=mesh,
        in_specs=(P("section", "expert", None), P("section", "expert", None, None), P("section", "expert", None),
                  P("section", "expert", None), P("section", "expert", None, None), P("section", None, None)),
        out_specs=(P("section", "expert", None, None), P("section", "expert", None)), check_vma=False)
```

```python
import functools
import jax
import jax.numpy as jnp
from jax import lax
from jax.experimental import pallas as pl
from jax.experimental.pallas import tpu as pltpu
from jax.sharding import PartitionSpec as P

MESH = pl.DeviceIdType.MESH
CAP = 24
ORDERS = ((0, 1, 2), (1, 2, 0), (2, 0, 1))
STRIDE = (16, 4, 1)
GB = (10, 12, 10)
HB = (2, 3, 3)


def starts(blocks):
    return tuple(128 * sum(blocks[:i]) for i in range(len(blocks)))


def comm_kernel(routes, scores, router, grad, hidden, down, F, HR, handed, hid, HV, wv, gch, g2, ds, dr, hnd, codes_s, score_s, tab, rc, U0, U1, U2, lv0, lv1, lv2,
                gb0, gb1, gb2, sc0, sc1, sc2, ha0, ha1, ha2, hb0, hb1, hb2, hc0, hc1, hc2,
                lsem, gas, gar, gbs, gbr, gcs, gcr, gcl, has, har, hbs, hbr, hcs, hcr, gls, wsem, dss, drs, hos, lvs, tss, trs):
    gb, sc, ha, hb, hc = (gb0, gb1, gb2), (sc0, sc1, sc2), (ha0, ha1, ha2), (hb0, hb1, hb2), (hc0, hc1, hc2)
    e = lax.axis_index("expert")
    co = (e // 16, (e // 4) % 4, e % 4)
    gcol, hcol = starts(GB), starts(HB)
    U, lv = (U0, U1, U2), (lv0, lv1, lv2)

    def wrap(v):
        return lax.rem(v + 4, 4)

    def peer(axis, delta):
        c = list(co)
        c[axis] = wrap(co[axis] + delta)
        return {"expert": c[0] * 16 + c[1] * 4 + c[2]}

    def rcopy(src, dst, ss, rs, axis, delta):
        return pltpu.make_async_remote_copy(src_ref=src, dst_ref=dst, send_sem=ss, recv_sem=rs,
                                            device_id=peer(axis, delta), device_id_type=MESH)

    def plane(p, da, db):
        A, B, C = ORDERS[p]
        c = list(co)
        c[A], c[B] = wrap(co[A] + da), wrap(co[B] + db)
        return c, {"expert": c[0] * 16 + c[1] * 4 + c[2]}

    barrier = pltpu.get_barrier_semaphore()
    for axis in range(3):
        for d in (1, 2, 3):
            pl.semaphore_signal(barrier, inc=1, device_id=peer(axis, d), device_id_type=MESH)

    sends = []

    def go(cp):
        cp.start()
        sends.append(cp)
        return cp

    loads = []
    for p, (A, B, C) in enumerate(ORDERS):
        gw = GB[p] * 128
        own = gb[p].at[co[B], co[A]]
        l0 = pltpu.make_async_copy(grad.at[:, pl.ds(gcol[p], gw)], own.at[:, pl.ds(0, gw)], lsem.at[p, 0])
        l0.start()
        loads.append(l0)
    hload = pltpu.make_async_copy(hidden, hid, lsem.at[0, 1])
    hload.start()
    wload = pltpu.make_async_copy(down, wv, wsem.at[0])
    wload.start()

    def ring(p, axis, slot_of, sems, semr, idx):
        gw = GB[p] * 128
        half = (gw // 256) * 128
        def cp(i, src_delta, cols, delta):
            ref = slot_of(src_delta)
            if cols is not None:
                ref = ref.at[:, pl.ds(*cols)]
            return rcopy(ref, ref, sems.at[idx + (i,)], semr.at[idx + (i,)], axis, delta)
        return (cp(0, 0, None, 1), cp(1, 0, None, -1), cp(2, -1, (0, half), 1), cp(3, 1, (half, gw - half), -1))

    acp, bcp = [], {}
    for p, (A, B, C) in enumerate(ORDERS):
        acp.append(ring(p, A, lambda d, p=p, A=A, B=B: gb[p].at[co[B], wrap(co[A] + d)], gas, gar, (p,)))
        for k, da in enumerate((0, -1, 1, 2)):
            bcp[p, k] = ring(p, B, lambda d, p=p, A=A, B=B, da=da: gb[p].at[wrap(co[B] + d), wrap(co[A] + da)], gbs, gbr, (p, k))
    pl.semaphore_wait(barrier, 9)
    for p in range(3):
        loads[p].wait()
        go(acp[p][0]); go(acp[p][1])
    for p in range(3):
        go(bcp[p, 0][0]); go(bcp[p, 0][1])

    f32, bf = jnp.float32, jnp.bfloat16
    ri = routes[...].astype(f32)
    st = scores[...]
    tot = jnp.sum(st, axis=0, keepdims=True)
    low = (st / tot).astype(bf)
    eio = lax.broadcasted_iota(jnp.int32, (64, 128), 0).astype(f32)
    member = jnp.zeros((64, 128), f32)
    score_e = jnp.zeros((64, 128), f32)
    for k in range(8):
        hit = eio == ri[k:k + 1, :]
        member = member + jnp.where(hit, 1.0, 0.0)
        score_e = score_e + jnp.where(hit, st[k:k + 1, :], 0.0)
    before = lax.broadcasted_iota(jnp.int32, (128, 128), 0) < lax.broadcasted_iota(jnp.int32, (128, 128), 1)
    rank = jnp.dot(member.astype(bf), jnp.where(before, 1.0, 0.0).astype(bf), preferred_element_type=f32)
    code_e = jnp.where(member > 0.0, rank, -1.0)
    codes_s[...] = code_e
    score_s[...] = score_e
    for k in range(64):
        tab[k // 16, (k // 4) % 4, k % 4] = code_e[k:k + 1, :]

    slots = jnp.concatenate([jnp.sum(jnp.where(eio == ri[k:k + 1, :], rank, 0.0), axis=0, keepdims=True) for k in range(8)], axis=0)
    n8 = lax.broadcasted_iota(jnp.int32, (128, 1024), 1) // 8
    spread = jnp.where(n8 == lax.broadcasted_iota(jnp.int32, (128, 1024), 0), 1.0, 0.0).astype(bf)
    mine = lax.broadcasted_iota(jnp.int32, (8, 1024), 1) % 8 == lax.broadcasted_iota(jnp.int32, (8, 1024), 0)

    def lanes(v):
        return jnp.sum(jnp.where(mine, jnp.dot(v.astype(bf), spread, preferred_element_type=f32), 0.0), axis=0, keepdims=True)
    tgt = CAP * lanes(ri) + lanes(slots)
    wgt = lanes(low)
    hload.wait()

    for p, (A, B, C) in enumerate(ORDERS):
        hw = HB[p] * 128
        r = lax.broadcasted_iota(jnp.int32, (16 * CAP, 1), 0)
        dB = (r >= 4 * CAP).astype(jnp.int32) + (r >= 8 * CAP).astype(jnp.int32) + (r >= 12 * CAP).astype(jnp.int32)
        r1 = r - dB * (4 * CAP)
        dC = (r1 >= CAP).astype(jnp.int32) + (r1 >= 2 * CAP).astype(jnp.int32) + (r1 >= 3 * CAP).astype(jnp.int32)
        slot = r1 - dC * CAP
        base = CAP * (dB * STRIDE[B] + dC * STRIDE[C]) + slot
        for d in (1, 3, 2, 0):
            code = base + CAP * STRIDE[A] * wrap(co[A] + d)
            pick = jnp.where(code.astype(f32) == tgt, wgt, 0.0).astype(jnp.bfloat16)
            rows = jnp.dot(pick, hid[:, hcol[p]:hcol[p] + hw], preferred_element_type=jnp.float32)
            rows = rows.reshape(4, 4, CAP, hw).astype(jnp.bfloat16)
            if d == 0:
                for j in range(4):
                    hb[p][j, co[A]] = rows[j]
            else:
                ha[p][d - 1] = rows
                go(rcopy(ha[p].at[d - 1], hb[p].at[:, co[A]], has.at[p, d - 1], har.at[p, d - 1], A, d))
    hacp = {}
    for p, (A, B, C) in enumerate(ORDERS):
        for d in (1, 2, 3):
            hacp[p, d] = rcopy(ha[p].at[d - 1], hb[p].at[:, wrap(co[A] - d)], has.at[p, d - 1], har.at[p, d - 1], A, d)

    for p in range(3):
        acp[p][0].wait_recv(); go(acp[p][2])
        acp[p][1].wait_recv(); go(acp[p][3])
    for p in range(3):
        for k in (1, 2):
            go(bcp[p, k][0]); go(bcp[p, k][1])
    for p in range(3):
        acp[p][2].wait_recv(); acp[p][3].wait_recv()
        go(bcp[p, 3][0]); go(bcp[p, 3][1])

    for p, (A, B, C) in enumerate(ORDERS):
        for da in range(4):
            for db in range(4):
                c, dev = plane(p, da, db)
                idx = list(c)
                if da == 0 and db == 0:
                    for k in range(4):
                        idx[C] = k
                        rc[p, co[B] * 4 + co[A], k] = tab[idx[0], idx[1], idx[2]]
                    continue
                idx[C] = slice(None)
                pltpu.make_async_remote_copy(src_ref=tab.at[idx[0], idx[1], idx[2]], dst_ref=rc.at[p, co[B] * 4 + co[A]],
                                             send_sem=tss.at[p], recv_sem=trs.at[p], device_id=dev, device_id_type=MESH).start()

    j = lax.broadcasted_iota(jnp.int32, (4 * CAP, 1), 0)
    dCj = (j >= CAP).astype(jnp.int32) + (j >= 2 * CAP).astype(jnp.int32) + (j >= 3 * CAP).astype(jnp.int32)
    slotj = (j - dCj * CAP).astype(jnp.float32)

    def pack(p, db):
        A, B, C = ORDERS[p]
        gw = GB[p] * 128
        bb = wrap(co[B] + db)

        def one(a, carry):
            codes = jnp.concatenate([jnp.broadcast_to(rc[p, bb * 4 + a, wrap(co[C] + dc)], (CAP, 128)) for dc in range(4)], axis=0)
            sel = jnp.where(codes == slotj, 1.0, 0.0).astype(jnp.bfloat16)
            rows = jnp.dot(sel, gb[p][bb, a, :, 0:gw], preferred_element_type=jnp.float32)
            rows = rows.reshape(4, CAP, gw).astype(jnp.bfloat16)
            for dc in range(4):
                if db == 2 and dc == 0:
                    if A < C:
                        lv[p][a, co[C]] = rows[0]
                    else:
                        lv[p][co[C], a] = rows[0]
                else:
                    sc[p][dc, db % 4, a] = rows[dc]
            return carry
        lax.fori_loop(0, 4, one, 0)
        for dc in (1, 3, 2):
            go(rcopy(sc[p].at[dc, db % 4], fdst(p, db, 0), gcs.at[p, db % 4, dc - 1], gcr.at[p, db % 4, dc - 1], C, dc))
        if db != 2:
            cp = pltpu.make_async_copy(sc[p].at[0, db % 4], fdst(p, db, 0), gcl.at[p, db % 4])
            cp.start()
            locals_[p, db % 4] = cp

    def fdst(p, db, d):
        A, B, C = ORDERS[p]
        if db == 2:
            c = wrap(co[C] - d)
            return lv[p].at[:, c] if A < C else lv[p].at[c, :]
        idx = [None, None, None]
        idx[A] = slice(None)
        idx[B] = wrap(co[B] + db)
        idx[C] = wrap(co[C] - d)
        return F.at[idx[0], idx[1], idx[2], :, pl.ds(gcol[p], GB[p] * 128)]

    def hdst(p, bb, d):
        A, B, C = ORDERS[p]
        idx = [None, None, None]
        idx[A] = slice(None)
        idx[B] = bb
        idx[C] = wrap(co[C] - d)
        return HV.at[idx[0], idx[1], idx[2], :, pl.ds(hcol[p], HB[p] * 128)]

    locals_ = {}
    hbcp = {}
    for p, (A, B, C) in enumerate(ORDERS):
        for d in (1, 3, 2):
            hacp[p, d].wait_recv()
        for d in (1, 3, 2):
            hbcp[p, d] = go(rcopy(hb[p].at[wrap(co[B] + d)], hc[p].at[d - 1], hbs.at[p, d - 1], hbr.at[p, d - 1], B, d))
    for p in range(3):
        pltpu.make_async_copy(rc.at[p, pl.ds(0, 15)], rc.at[p, pl.ds(0, 15)], trs.at[p]).wait()
        pack(p, 0)
    for k in range(4):
        for p in range(3):
            bcp[p, k][0].wait_recv(); go(bcp[p, k][2])
            bcp[p, k][1].wait_recv(); go(bcp[p, k][3])

    def hidden_c(p, d):
        A, B, C = ORDERS[p]
        bb = wrap(co[B] - d)
        for dc in (1, 3, 2, 0):
            cs = wrap(co[C] + dc)
            src = hb[p].at[co[B], :, cs] if d == 0 else hc[p].at[d - 1, :, cs]
            if dc == 0:
                dst = hdst(p, bb, 0)
                for a in range(4):
                    dst[a] = src[a]
            else:
                go(rcopy(src, hdst(p, bb, 0), hcs.at[p, d, dc - 1], hcr.at[p, d, dc - 1], C, dc))
    for p in range(3):
        hidden_c(p, 0)
    for p in range(3):
        for d in (1, 3, 2):
            hbcp[p, d].wait_recv()
            hidden_c(p, d)
    for p in range(3):
        pack(p, -1)
    for p in range(3):
        pack(p, 1)
    for p in range(3):
        for k in range(4):
            bcp[p, k][2].wait_recv(); bcp[p, k][3].wait_recv()
        pack(p, 2)
    for p, (A, B, C) in enumerate(ORDERS):
        for d in range(4):
            for dc in (1, 3, 2):
                src = hc[p].at[max(d - 1, 0), :, 0]
                rcopy(src, hdst(p, wrap(co[B] - d), dc), hcs.at[p, d, dc - 1], hcr.at[p, d, dc - 1], C, dc).wait_recv()
    hout = pltpu.make_async_copy(HV, HR, hos.at[0])
    hout.start()
    wload.wait()

    def rest(p):
        return tuple(ax for ax in range(3) if ax != ORDERS[p][1])

    def at_b(ref, p, bb):
        idx = [slice(None)] * 3
        idx[ORDERS[p][1]] = bb
        return ref.at[idx[0], idx[1], idx[2]]

    chunks = [(p, db) for db in (0, -1, 1) for p in range(3)]

    def arrived(p, db):
        for dc in (1, 3, 2):
            rcopy(sc[p].at[dc, db % 4], fdst(p, db, dc), gcs.at[p, db % 4, dc - 1], gcr.at[p, db % 4, dc - 1], ORDERS[p][2], dc).wait_recv()
        if db != 2:
            locals_[p, db % 4].wait()

    for p in range(3):
        view = at_b(HV, p, wrap(co[ORDERS[p][1]] + 2))
        for i in range(4):
            g2[i * 96:(i + 1) * 96, 0:1024] = view[i].astype(f32).reshape(96, 1024).astype(bf)

        def prod(ct, carry, p=p):
            cols = pl.ds(pl.multiple_of(ct * 256, 256), 256)
            wcols = pl.ds(pl.multiple_of(gcol[p] + ct * 256, 256), 256)
            u = jnp.dot(g2[:, 0:1024], wv[:, wcols], preferred_element_type=f32)
            U[p][:, :, :, cols] = u.reshape(4, 4, CAP, 256).astype(bf)
            return carry
        lax.fori_loop(0, GB[p] // 2, prod, 0)

    def load(n):
        p, db = chunks[n]
        bb = wrap(co[ORDERS[p][1]] + db)
        arrived(p, db)
        gw = GB[p] * 128
        cp = pltpu.make_async_copy(at_b(F, p, bb).at[:, :, :, pl.ds(gcol[p], gw)], gch.at[n % 2, :, :, :, pl.ds(0, gw)], gls.at[n % 2])
        cp.start()
        return cp

    def derive(n):
        p, db = chunks[n]
        gw = GB[p] * 128
        B = ORDERS[p][1]
        bb = wrap(co[B] + db)
        R1, R2 = rest(p)
        for i in range(4):
            g2[i * 96:(i + 1) * 96, 0:gw] = gch[n % 2, i, :, :, 0:gw].astype(f32).reshape(96, gw).astype(bf)
        hview = at_b(HV, p, bb)
        acc = jnp.zeros((384, 128), f32)
        for f in range(4):
            proj = lax.dot_general(g2[:, 0:gw], wv[f * 256:(f + 1) * 256, gcol[p]:gcol[p] + gw], (((1,), (1,)), ((), ())),
                                   preferred_element_type=f32)
            q = proj * hview[:, :, :, f * 256:(f + 1) * 256].astype(f32).reshape(384, 256)
            acc = acc + q[:, 0:128] + q[:, 128:256]
        give(p, db, acc)

    def give(p, db, acc):
        B = ORDERS[p][1]
        bb = wrap(co[B] + db)
        R1, R2 = rest(p)
        pad = jnp.concatenate([acc.reshape(16, CAP, 128), jnp.zeros((16, 8, 128), f32)], axis=1).reshape(512, 128)
        row = jnp.sum(jnp.transpose(pad), axis=0, keepdims=True)
        for i in range(4):
            ds[p, db % 4, i] = row[:, i * 128:(i + 1) * 128]
        for d1 in range(4):
            for d2 in range(4):
                i = wrap(co[R1] + d1)
                if (db, d1, d2) == (0, 0, 0):
                    dr[p, e] = ds[p, 0, i]
                    continue
                c = [None] * 3
                c[R1], c[R2], c[B] = i, wrap(co[R2] + d2), bb
                pltpu.make_async_remote_copy(src_ref=ds.at[p, db % 4, i], dst_ref=dr.at[p, e], send_sem=dss.at[p], recv_sem=drs.at[p],
                                             device_id={"expert": c[0] * 16 + c[1] * 4 + c[2]}, device_id_type=MESH).start()

    cur = load(0)
    for n in range(9):
        nxt = load(n + 1) if n < 8 else None
        cur.wait()
        derive(n)
        cur = nxt
    lcps = []
    for p in range(3):
        arrived(p, 2)
        cp = pltpu.make_async_copy(lv[p], at_b(F, p, wrap(co[ORDERS[p][1]] + 2)).at[:, :, :, pl.ds(gcol[p], GB[p] * 128)], lvs.at[p])
        cp.start()
        lcps.append(cp)
        quads = []
        for i in range(4):
            t = jnp.zeros((4, CAP, 128), f32)
            for k in range(GB[p]):
                cols = slice(k * 128, (k + 1) * 128)
                t = t + U[p][i, :, :, cols].astype(f32) * lv[p][i, :, :, cols].astype(f32)
            quads.append(t.reshape(96, 128))
        give(p, 2, jnp.concatenate(quads, axis=0))

    home = jnp.zeros((64, 128), f32)
    window = lax.broadcasted_iota(jnp.int32, (64, 128), 1) // 32
    for p in range(3):
        pltpu.make_async_copy(dr.at[p, pl.ds(0, 63)], dr.at[p, pl.ds(0, 63)], drs.at[p]).wait()
        home = home + jnp.where(window == co[rest(p)[1]], dr[p].reshape(64, 128), 0.0)
    home = home + pltpu.roll(home, 64, 1)
    home = home + pltpu.roll(home, 32, 1)
    code_e = codes_s[...]
    score_e = score_s[...]
    rd = jnp.zeros((64, 128), f32)
    for s in range(CAP):
        rd = rd + jnp.where(code_e == float(s), home[:, s:s + 1], 0.0)
    tot = jnp.sum(score_e, axis=0, keepdims=True)
    weight = score_e / tot
    on = code_e >= 0.0
    rd = jnp.where(on, rd / jnp.where(on, weight.astype(bf).astype(f32), 1.0), 0.0)
    center = jnp.sum(weight * rd, axis=0, keepdims=True)
    logit = score_e * (1.0 - score_e) / tot * (rd - center)
    lt = jnp.transpose(logit).astype(bf)
    hcps = []
    for p, (A, B, C) in enumerate(ORDERS):
        gw = GB[p] * 128
        for c0 in range(0, gw, gw // 2):
            add = jnp.dot(lt, router[:, gcol[p] + c0:gcol[p] + c0 + gw // 2], preferred_element_type=f32)
            hnd[:, gcol[p] + c0:gcol[p] + c0 + gw // 2] = (gb[p][co[B], co[A], :, c0:c0 + gw // 2].astype(f32) + add).astype(bf)
        cols = pl.ds(gcol[p], gw)
        cp = pltpu.make_async_copy(hnd.at[:, cols], handed.at[:, cols], gls.at[p])
        cp.start()
        hcps.append(cp)
    for p in range(3):
        pltpu.make_async_copy(dr.at[p, pl.ds(0, 63)], dr.at[p, pl.ds(0, 63)], dss.at[p]).wait()
    for p in range(3):
        pltpu.make_async_copy(rc.at[p, pl.ds(0, 15)], rc.at[p, pl.ds(0, 15)], tss.at[p]).wait()
    for cp in lcps:
        cp.wait()
    hout.wait()
    for cp in sends:
        cp.wait_send()
    for cp in hcps:
        cp.wait()


def exchange(routes, scores, router, grad, hidden, down):
    bf, f32 = jnp.bfloat16, jnp.float32
    V = pltpu.VMEM
    D = pltpu.SemaphoreType.DMA
    any_ = pl.BlockSpec(memory_space=pl.ANY)
    vm = pl.BlockSpec(memory_space=pltpu.VMEM)
    gmax = max(GB) * 128
    F, HR, handed = pl.pallas_call(
        comm_kernel,
        out_shape=(jax.ShapeDtypeStruct((4, 4, 4, CAP, 4096), bf), jax.ShapeDtypeStruct((4, 4, 4, CAP, 1024), bf),
                   jax.ShapeDtypeStruct((128, 4096), bf)),
        in_specs=[vm, vm, vm, any_, any_, any_], out_specs=(any_, any_, any_),
        scratch_shapes=[V((1024, 1024), bf), V((4, 4, 4, CAP, 1024), bf), V((1024, 4096), bf), V((2, 4, 4, CAP, gmax), bf),
                        V((384, gmax), bf), V((3, 4, 4, 1, 128), f32), V((3, 64, 1, 128), f32), V((128, 4096), bf),
                        V((64, 128), f32), V((64, 128), f32), V((4, 4, 4, 1, 128), f32), V((3, 16, 4, 1, 128), f32)]
        + [V((4, 4, CAP, g * 128), bf) for g in GB] * 2
        + [V((4, 4, 128, g * 128), bf) for g in GB]
        + [V((4, 4, 4, CAP, g * 128), bf) for g in GB]
        + [V((3, 4, 4, CAP, h * 128), bf) for h in HB]
        + [V((4, 4, 4, CAP, h * 128), bf) for h in HB]
        + [V((3, 4, 4, CAP, h * 128), bf) for h in HB]
        + [D((3, 2)), D((3, 4)), D((3, 4)), D((3, 4, 4)), D((3, 4, 4)), D((3, 4, 3)), D((3, 4, 3)), D((3, 4)),
           D((3, 3)), D((3, 3)), D((3, 3)), D((3, 3)), D((3, 4, 3)), D((3, 4, 3)),
           D((3,)), D((1,)), D((3,)), D((3,)), D((1,)), D((3,)), D((3,)), D((3,))],
        compiler_params=pltpu.CompilerParams(has_side_effects=True, collective_id=0, vmem_limit_bytes=67043328),
    )(routes, scores, router, grad, hidden, down)
    return F.reshape(64 * CAP, 4096), HR.reshape(64 * CAP, 1024), handed


def body(grad_out, saved_hidden, routes, scores, down_weight, router):
    n_tokens, n_routes, hidden_width = saved_hidden.shape[1:]
    hidden_flat = saved_hidden[0].reshape(n_tokens * n_routes, hidden_width)
    grad_recv, hidden_recv, inp = exchange(routes[0].T, scores[0].T, router[0], grad_out[0], hidden_flat, down_weight[0, 0])
    handed = lax.ppermute(inp, "section", [(0, 1), (1, 0)])
    weight_out = lax.dot_general(hidden_recv, grad_recv, (((0,), (0,)), ((), ())), preferred_element_type=jnp.float32).astype(jnp.bfloat16)
    return weight_out[None, None], handed[None]


def solution(mesh):
    return jax.shard_map(
        body, mesh=mesh,
        in_specs=(P("section", "expert", None), P("section", "expert", None, None), P("section", "expert", None),
                  P("section", "expert", None), P("section", "expert", None, None), P("section", None, None)),
        out_specs=(P("section", "expert", None, None), P("section", "expert", None)), check_vma=False)
```
